128 devices in a mesh: rep: 2 (over core), dp: 64 (over x, y, z).
Axes of the slice: x: 4, y: 4, z: 4, core: 2. Of those that a mesh axis runs over, the one named last changes fastest.
Arguments:
- g_w_gate: bfloat16 [128, 2, 640, 3200], P(('rep', 'dp')), parts along dimension 0
- g_w_up: bfloat16 [128, 2, 640, 3200], P(('rep', 'dp')), parts along dimension 0
- g_w_down: bfloat16 [128, 2, 3200, 640], P(('rep', 'dp')), parts along dimension 0
- w_gate: bfloat16 [2, 640, 3200], replicated
- w_up: bfloat16 [2, 640, 3200], replicated
- w_down: bfloat16 [2, 3200, 640], replicated
- m_w_gate: float32 [2, 640, 3200], P(None, 'dp')
- m_w_up: float32 [2, 640, 3200], P(None, 'dp')
- m_w_down: float32 [2, 3200, 640], P(None, 'dp')
- v_w_gate: float32 [2, 640, 3200], P(None, 'dp')
- v_w_up: float32 [2, 640, 3200], P(None, 'dp')
- v_w_down: float32 [2, 3200, 640], P(None, 'dp')
Outputs:
- output 1: bfloat16 [4, 640, 3200], P('rep'), parts along dimension 0
- output 2: bfloat16 [4, 640, 3200], P('rep'), parts along dimension 0
- output 3: bfloat16 [4, 3200, 640], P('rep'), parts along dimension 0
- output 4: float32 [4, 640, 3200], P('rep', 'dp'), parts along dimension 0
- output 5: float32 [4, 640, 3200], P('rep', 'dp'), parts along dimension 0
- output 6: float32 [4, 3200, 640], P('rep', 'dp'), parts along dimension 0
- output 7: float32 [4, 640, 3200], P('rep', 'dp'), parts along dimension 0
- output 8: float32 [4, 640, 3200], P('rep', 'dp'), parts along dimension 0
- output 9: float32 [4, 3200, 640], P('rep', 'dp'), parts along dimension 0
There are 2 independent parts. The reference program is written for one: setup_inputs(seed, part) draws one part's arguments, and reference() takes and returns one part's arrays. A program takes and returns all parts, laid end to end along the dimension named above; an argument that names none is the same for every part.
All inputs are finite; a program needn't handle non-finite values.
Results may differ from the reference program's by a relative error of at most 0.022.
Values are sent between devices in bfloat16 or wider.
A program may use at most 1.5 GiB of HBM per device.

```python
import jax
import jax.numpy as jnp
from jax import lax

DEVICES = 64
D = 640
FF = 3200
LAYERS = 2
NAMES = ("w_gate", "w_up", "w_down")
SHAPES = {"w_gate": (LAYERS, D, FF), "w_up": (LAYERS, D, FF), "w_down": (LAYERS, FF, D)}


def setup_inputs(seed: int = 0, part: int = 0) -> dict:
    kz, *keys = jax.random.split(jax.random.key(seed), 1 + 5 * len(NAMES))
    loud = 2.0 ** jax.random.uniform(kz, (), jnp.float32, -1.0, 1.0)
    drawn = {}
    for name, key, both in zip(NAMES, keys[:3], keys[3:6], strict=True):
        own = jax.random.normal(jax.random.fold_in(key, part), (DEVICES, *SHAPES[name]), jnp.float32)
        shared = jax.random.normal(jax.random.fold_in(both, part), SHAPES[name], jnp.float32)
        drawn["g_" + name] = (loud * (0.7 * shared / DEVICES + 0.7 * own * DEVICES**-0.5)).astype(jnp.bfloat16)
    for name, key in zip(NAMES, keys[6:9], strict=True):
        drawn[name] = (jax.random.normal(key, SHAPES[name], jnp.float32) * SHAPES[name][1] ** -0.5).astype(jnp.bfloat16)
    for name, key in zip(NAMES, keys[9:12], strict=True):
        drawn["m_" + name] = loud * 0.5 * jax.random.normal(key, SHAPES[name], jnp.float32)
    for name, key in zip(NAMES, keys[12:15], strict=True):
        drawn["v_" + name] = loud * loud * jax.random.uniform(key, SHAPES[name], jnp.float32, 0.5, 1.5)
    return drawn


def adamw(w, m, v, g):
    m = 0.9 * m + 0.1 * g
    v = 0.95 * v + 0.05 * g * g
    step = m * lax.rsqrt(v + 1e-8) + 0.1 * w
    return (w - 0.02 * step).astype(jnp.bfloat16), m, v


def reference(g_w_gate, g_w_up, g_w_down, w_gate, w_up, w_down, m_w_gate, m_w_up, m_w_down, v_w_gate, v_w_up, v_w_down):
    def total(terms):
        return lax.scan(lambda so_far, term: (so_far + term.astype(jnp.float32), None), jnp.zeros(terms.shape[1:], jnp.float32), terms)[0]

    gradients = [total(terms).astype(jnp.bfloat16).astype(jnp.float32) for terms in (g_w_gate, g_w_up, g_w_down)]
    new = [
        adamw(w.astype(jnp.float32), m, v, g)
        for w, m, v, g in zip((w_gate, w_up, w_down), (m_w_gate, m_w_up, m_w_down), (v_w_gate, v_w_up, v_w_down), gradients, strict=True)
    ]
    return tuple(one[which] for which in range(3) for one in new)
```

```python
import functools
import heapq

import jax
import jax.numpy as jnp
from jax import lax
from jax.experimental import pallas as pl
from jax.experimental.pallas import tpu as pltpu
from jax.sharding import PartitionSpec as P

BF16, F32 = jnp.bfloat16, jnp.float32
MESH = pl.DeviceIdType.MESH
SIGN = (1, -1)
ORDER = (((0, 1, 2), (0, 1, 2)), ((1, 0, 2), (1, 0, 2)), ((2, 0, 1), (2, 1, 0)))
FLOWS = tuple((w, l) for w in range(3) for l in range(2))


def adamw(w, m, v, g):
    m = 0.9 * m + 0.1 * g
    v = 0.95 * v + 0.05 * g * g
    step = m * lax.rsqrt(v + 1e-8) + 0.1 * w
    return (w - 0.02 * step).astype(BF16), m, v


def in_order(first, tasks, sends):
    rate, trip = 46.6e3, 2.2
    free, arrived, done, order = {}, {}, {}, []

    def send(message, at):
        link, size = sends[message]
        start = max(free.get(link, 0.0), at)
        free[link] = start + size / rate
        arrived[message] = free[link] + trip

    for message in first:
        send(message, 0.0)
    now, left = 0.0, dict(tasks)
    while left:
        ready = []
        for place, (task, (message, before, _, _)) in enumerate(left.items()):
            if message in arrived and all(b in done for b in before):
                ready.append((max([arrived[message]] + [done[b] for b in before]), place, task))
        at, _, task = min(ready)
        now = max(now, at) + left[task][2]
        done[task] = now
        for message in left.pop(task)[3]:
            send(message, now)
        order.append(task)
    return order


def place():
    me = lax.axis_index("dp")
    return lax.div(me, 16), lax.rem(lax.div(me, 4), 4), lax.rem(me, 4)


def towards(at, axis, sign):
    to = list(at)
    to[axis] = lax.rem(at[axis] + 4 + sign, 4)
    return {"dp": to[0] * 16 + to[1] * 4 + to[2]}


def ring(p, sign, steps):
    return lax.rem(p + 8 - sign * steps, 4)


def meet(at):
    barrier = pltpu.get_barrier_semaphore()
    for axis in range(3):
        for sign in SIGN:
            pl.semaphore_signal(barrier, inc=1, device_id=towards(at, axis, sign), device_id_type=MESH)
    pl.semaphore_wait(barrier, 6)


def rows8(i, size):
    return pl.ds(pl.multiple_of(i, 8), size)


def pieces(ref, body):
    if len(ref.shape) == 3:
        steps, index = ref.shape[0], lambda j: (j,)
    elif ref.shape[1] == 3200:
        steps, index = 5, lambda j: (slice(None), pl.ds(pl.multiple_of(j * 640, 128), 640))
    else:
        return body((slice(None), slice(None)))
    lax.fori_loop(0, steps, lambda j, _: (body(index(j)), 0)[1], 0)


def add_to(out, a, b):
    def one(i):
        out[i] = (a[i].astype(F32) + b[i].astype(F32)).astype(BF16)

    pieces(out, one)


CELL = (40 * 3200 * 2, 40 * 3200 * 2, 4 * 56 * 640 * 2)
LAST = (16 * 3200 * 2, 16 * 3200 * 2, 56 * 640 * 2)


def sum_order():
    tasks, sends, first = {}, {}, []
    for t in range(3):
        for k in range(4):
            for w, l in FLOWS:
                a, b, c = ORDER[w][l]
                m = ("a", w, l, t, k)
                sends[m] = ((a, l), CELL[w])
                if t == 0:
                    first.append(m)
                nxt = [("a", w, l, t + 1, k)] if t < 2 else [("b", w, l, 0)] if k == 0 else []
                tasks[m] = (m, [], CELL[w] / 2 / 1024 * 5 / 1900, nxt)
    for w, l in FLOWS:
        a, b, c = ORDER[w][l]
        for t in range(3):
            m = ("b", w, l, t)
            sends[m] = ((b, l), CELL[w])
            tasks[m] = (m, [("a", w, l, 2, t + 1)], CELL[w] / 2 / 1024 * 5 / 1900, [("b", w, l, t + 1)] if t < 2 else [("c", w, l, 0)])
            m = ("c", w, l, t)
            sends[m] = ((c, l), LAST[w])
            tasks[m] = (m, [("b", w, l, 2)], LAST[w] / 2 / 1024 * 5 / 1900, [("c", w, l, t + 1)] if t < 2 else [])
    return in_order(first, tasks, sends)


def sum_kernel(*refs):
    terms, outs = refs[:3], refs[3:6]
    r1, mine, r2, r3 = refs[6:9], refs[9:12], refs[12:15], refs[15:18]
    load_sem, a_send, a_recv, b_send, b_recv, c_send, c_recv = refs[18:]
    at = place()

    def source(w, l, block, k):
        a, b, _ = ORDER[w][l]
        chunk = ring(at[b], SIGN[l], 1 + k)
        if w < 2:
            i, j = (block, chunk) if a == 0 else (chunk, block)
            return terms[w].at[l, i, j]
        window = rows8(block * 48, 56)
        return terms[w].at[l, chunk, :, window, :] if b == 0 else terms[w].at[l, :, chunk, window, :]

    def load(w, l, t, k):
        block = ring(at[ORDER[w][l][0]], SIGN[l], 2 + t)
        return pltpu.make_async_copy(source(w, l, block, k), mine[w].at[l, t, k], load_sem.at[w, l, t, k])

    def last(w, l, t):
        block = ring(at[ORDER[w][l][2]], SIGN[l], 2 + t)
        return r2[w].at[l, 2, rows8(block * 8, 16), :] if w < 2 else r2[w].at[l, 2, block]

    def message(name, w, l, t, k=0):
        a, b, c = ORDER[w][l]
        if name == "a":
            src = source(w, l, ring(at[a], SIGN[l], 1), k) if t == 0 else r1[w].at[l, t - 1, k]
            dst, sems, axis = r1[w].at[l, t, k], (a_send.at[w, l, t, k], a_recv.at[w, l, t, k]), a
        elif name == "b":
            src = r1[w].at[l, 2, 0] if t == 0 else r2[w].at[l, t - 1]
            dst, sems, axis = r2[w].at[l, t], (b_send.at[w, l, t], b_recv.at[w, l, t]), b
        else:
            src = last(w, l, -1) if t == 0 else r3[w].at[l, t - 1]
            dst, sems, axis = r3[w].at[l, t], (c_send.at[w, l, t], c_recv.at[w, l, t]), c
        return pltpu.make_async_remote_copy(
            src_ref=src, dst_ref=dst, send_sem=sems[0], recv_sem=sems[1], device_id=towards(at, axis, SIGN[l]), device_id_type=MESH
        )

    order = sum_order()
    for name, *key in order:
        if name == "a":
            load(*key).start()
    meet(at)
    for k in range(4):
        for w, l in FLOWS:
            message("a", w, l, 0, k).start()
    for name, w, l, t, *k in order:
        message(name, w, l, t, *k).wait_recv()
        if name == "a":
            load(w, l, t, *k).wait()
            to = r1[w].at[l, t, k[0]]
            add_to(to, to, mine[w].at[l, t, k[0]])
            if t < 2:
                message("a", w, l, t + 1, *k).start()
            elif k[0] == 0:
                message("b", w, l, 0).start()
        elif name == "b":
            to = r2[w].at[l, t]
            add_to(to, to, r1[w].at[l, 2, t + 1])
            message(*(("b", w, l, t + 1) if t < 2 else ("c", w, l, 0))).start()
        else:
            to = r3[w].at[l, t] if t < 2 else outs[w].at[l]
            add_to(to, r3[w].at[l, t], last(w, l, t))
            if t < 2:
                message("c", w, l, t + 1).start()
    for name, *key in order:
        message(name, *key).wait_send()


def summed(terms):
    cells = ((40, 3200), (40, 3200), (4, 56, 640))
    ends = ((16, 3200), (16, 3200), (56, 640))
    dma = pltpu.SemaphoreType.DMA
    return pl.pallas_call(
        sum_kernel,
        out_shape=[jax.ShapeDtypeStruct((2, *e), BF16) for e in ends],
        in_specs=[pl.BlockSpec(memory_space=pltpu.HBM)] * 3,
        out_specs=[pl.BlockSpec(memory_space=pltpu.VMEM)] * 3,
        scratch_shapes=[
            *(pltpu.VMEM((2, 3, 4, *c), BF16) for c in cells),
            *(pltpu.VMEM((2, 3, 4, *c), BF16) for c in cells),
            *(pltpu.VMEM((2, 3, *c), BF16) for c in cells),
            *(pltpu.VMEM((2, 3, *e), BF16) for e in ends),
            dma((3, 2, 3, 4)),
            *(dma((3, 2, 3, 4)),) * 2,
            *(dma((3, 2, 3)),) * 4,
        ],
        compiler_params=pltpu.CompilerParams(collective_id=0, has_side_effects=True, vmem_limit_bytes=60 * 2**20),
        name="sum_terms",
    )(*terms)


def gather_order():
    tasks, sends, first = {}, {}, []
    for w, l in FLOWS:
        c, b, a = ORDER[w][l]
        first.append(("a", w, l, 0))
        for t in range(3):
            m = ("a", w, l, t)
            sends[m] = ((a, l), LAST[w])
            nxt = [("a", w, l, t + 1)] if t < 2 else [("b", w, l, 0), ("c", w, l, 0, 0)]
            tasks[m] = (m, [], 0.05 + (0.5 if t == 2 and w < 2 else 0), nxt)
            m = ("b", w, l, t)
            sends[m] = ((b, l), CELL[w])
            tasks[m] = (m, [("a", w, l, 2)], 0.05, ([("b", w, l, t + 1)] if t < 2 else []) + [("c", w, l, 0, t + 1)])
    for t in range(3):
        for k in range(4):
            for w, l in FLOWS:
                c, b, a = ORDER[w][l]
                m = ("c", w, l, t, k)
                sends[m] = ((c, l), CELL[w])
                tasks[m] = (m, [("b", w, l, 2)], 0.05, [("c", w, l, t + 1, k)] if t < 2 else [])
    return in_order(first, tasks, sends)


def gather_kernel(*refs):
    new, outs = refs[:3], refs[3:6]
    ends, cell, down = refs[6:8], refs[8:10], refs[10]
    own_sem, put_sem, a_send, a_recv, b_send, b_recv, c_send, c_recv = refs[11:]
    at = place()
    x, y, z = at

    def message(name, w, l, t, k=0):
        c, b, a = ORDER[w][l]
        s = SIGN[l]
        if name == "a":
            block = ring(at[a], s, t)
            if w < 2:
                dst = ends[w].at[l, block]
            else:
                dst = down.at[l, z, x, block] if a == 1 else down.at[l, z, block, y]
            src = new[w].at[l] if t == 0 else dst
            sems, axis = (a_send.at[w, l, t], a_recv.at[w, l, t]), a
        elif name == "b":
            block = ring(at[b], s, t)
            if w < 2:
                dst = outs[w].at[l, x, block] if b == 1 else outs[w].at[l, block, y]
                src = cell[w].at[l] if t == 0 else dst
            else:
                dst = src = down.at[l, z, :, block] if b == 1 else down.at[l, z, block]
            sems, axis = (b_send.at[w, l, t], b_recv.at[w, l, t]), b
        else:
            block, chunk = ring(at[c], s, t), ring(at[b], s, k)
            if w < 2:
                dst = outs[w].at[l, block, chunk] if c == 0 else outs[w].at[l, chunk, block]
                src = cell[w].at[l] if t == k == 0 else dst
            else:
                dst = src = down.at[l, block, :, chunk] if b == 1 else down.at[l, block, chunk]
            sems, axis = (c_send.at[w, l, t, k], c_recv.at[w, l, t, k]), c
        return pltpu.make_async_remote_copy(
            src_ref=src, dst_ref=dst, send_sem=sems[0], recv_sem=sems[1], device_id=towards(at, axis, s), device_id_type=MESH
        )

    def own(w, l):
        if w < 2:
            return pltpu.make_async_copy(cell[w].at[l], outs[w].at[l, x, y], own_sem.at[w, l])
        return None

    def keep(w, l):
        to = ends[w].at[l, z] if w < 2 else down.at[l, z, x, y]

        def one(i):
            to[i] = new[w].at[l][i]

        pieces(to, one)

    def join(w, l):
        def one(j, _):
            cols = pl.ds(pl.multiple_of(j * 640, 128), 640)
            row = lax.broadcasted_iota(jnp.int32, (8, 640), 0)
            top = [ends[w][l, i, 0:8, cols].astype(F32) for i in range(4)]
            low = [ends[w][l, i, 8:16, cols].astype(F32) for i in range(4)]
            tiles = [top[0], *(jnp.where(row < 2 * i, low[i - 1], top[i]) for i in (1, 2, 3)), low[3]]
            for i, tile in enumerate(tiles):
                cell[w][l, 8 * i : 8 * i + 8, cols] = tile.astype(BF16)
            return 0

        lax.fori_loop(0, 5, one, 0)

    def part(l, i, j, q):
        first = 0 if q == 0 else 8
        return down.at[l, q, i, j, first:56, :], outs[2].at[l, i, j, 48 * q + first : 48 * q + 56, :]

    def mend(l, k):
        b = ORDER[2][l][1]
        chunk = ring(at[b], SIGN[l], k)

        def one(n, _):
            i, j = (n, chunk) if b == 1 else (chunk, n)
            row = lax.broadcasted_iota(jnp.int32, (8, 640), 0)
            for q in range(3):
                low = down[l, q, i, j, 48:56, :].astype(F32)
                top = down[l, q + 1, i, j, 0:8, :].astype(F32)
                down[l, q, i, j, 48:56, :] = jnp.where(row < 2 * q + 2, low, top).astype(BF16)
            return 0

        lax.fori_loop(0, 4, one, 0)

    def put(l, k):
        b = ORDER[2][l][1]
        chunk = ring(at[b], SIGN[l], k)
        i, j = (slice(None), chunk) if b == 1 else (chunk, slice(None))
        return [pltpu.make_async_copy(*part(l, i, j, q), put_sem.at[l, k, q]) for q in range(4)]

    order, waited = gather_order(), set()
    meet(at)
    for w, l in FLOWS:
        message("a", w, l, 0).start()
    for w, l in FLOWS:
        keep(w, l)
    for name, w, l, t, *k in order:
        message(name, w, l, t, *k).wait_recv()
        if name == "a":
            if t < 2:
                message("a", w, l, t + 1).start()
            else:
                if w < 2:
                    join(w, l)
                message("b", w, l, 0).start()
                message("c", w, l, 0, 0).start()
                if w < 2:
                    own(w, l).start()
        elif name == "b":
            if t < 2:
                message("b", w, l, t + 1).start()
            message("c", w, l, 0, t + 1).start()
        elif t < 2:
            message("c", w, l, t + 1, *k).start()
        elif w == 2:
            over = [("c", w, l, step, *k) for step in range(3)]
            over += [("b", w, l, *k)] if k[0] < 3 else []
            over += [("a", w, l, step) for step in range(3)] if k[0] == 0 else []
            for sent in over:
                message(*sent).wait_send()
            waited.update(over)
            mend(l, *k)
            for copy in put(l, *k):
                copy.start()
    for task in order:
        if task not in waited:
            message(*task).wait_send()
    for w, l in FLOWS:
        if w < 2:
            own(w, l).wait()
    for l in range(2):
        for k in range(4):
            for copy in put(l, k):
                copy.wait()


def gathered(new):
    dma = pltpu.SemaphoreType.DMA
    shapes = ((2, 4, 4, 40, 3200),) * 2 + ((2, 4, 4, 200, 640),)
    return pl.pallas_call(
        gather_kernel,
        out_shape=[jax.ShapeDtypeStruct(s, BF16) for s in shapes],
        in_specs=[pl.BlockSpec(memory_space=pltpu.VMEM)] * 3,
        out_specs=[pl.BlockSpec(memory_space=pl.ANY)] * 3,
        scratch_shapes=[
            *(pltpu.VMEM((2, 4, 16, 3200), BF16),) * 2,
            *(pltpu.VMEM((2, 40, 3200), BF16),) * 2,
            pltpu.VMEM((2, 4, 4, 4, 56, 640), BF16),
            dma((2, 2)),
            dma((2, 4, 4)),
            *(dma((3, 2, 3)),) * 4,
            *(dma((3, 2, 3, 4)),) * 2,
        ],
        compiler_params=pltpu.CompilerParams(collective_id=1, has_side_effects=True, vmem_limit_bytes=20 * 2**20),
        name="gather_weights",
    )(*new)


def solution(mesh):
    def step(*arrays):
        terms, weights, m, v = (arrays[i : i + 3] for i in (0, 3, 6, 9))
        me = lax.axis_index("dp")
        z = lax.rem(me, 4)
        windows = summed([t.reshape(s) for t, s in zip(terms, ((2, 4, 4, 40, 3200),) * 2 + ((2, 4, 4, 200, 640),), strict=True)])
        gradients = [lax.dynamic_slice_in_dim(g, 2 * z, one.shape[1], 1).astype(F32) for g, one in zip(windows, m, strict=True)]
        own = [lax.dynamic_slice_in_dim(w, me * one.shape[1], one.shape[1], 1).astype(F32) for w, one in zip(weights, m, strict=True)]
        new = [adamw(w, m, v, g) for w, m, v, g in zip(own, m, v, gradients, strict=True)]
        put = [lax.dynamic_update_slice_in_dim(jnp.zeros_like(g), one[0], 2 * z, 1) for g, one in zip(windows, new, strict=True)]
        whole = [o.reshape(w.shape) for o, w in zip(gathered(put), weights, strict=True)]
        return (*whole, *(one[1] for one in new), *(one[2] for one in new))

    all_of, cut = P(None, None, None), P(None, "dp", None)
    return jax.shard_map(
        step,
        mesh=mesh,
        in_specs=(P(("rep", "dp"), None, None, None),) * 3 + (all_of,) * 3 + (cut,) * 6,
        out_specs=(P("rep", None, None),) * 3 + (P("rep", "dp", None),) * 6,
        check_vma=False,
    )
```

```python
import jax
import jax.numpy as jnp
from jax import lax
from jax.experimental import pallas as pl
from jax.experimental.pallas import tpu as pltpu
from jax.sharding import PartitionSpec as P

BF16, F32 = jnp.bfloat16, jnp.float32
MESH = pl.DeviceIdType.MESH
SIGN = (1, -1)
COLS = (((0, 3200),),) * 2 + (((0, 640),),)
HALVES = (0,)
XYZ, YXZ, ZXY, ZYX = (0, 1, 2), (1, 0, 2), (2, 0, 1), (2, 1, 0)
ORDER = (((XYZ, XYZ),) * 2, ((YXZ, YXZ),) * 2, ((ZXY, ZYX), (ZYX, ZXY)))
FLOWS = tuple((w, l, h) for h in HALVES for w in range(3) for l in range(2))
CELL, OWNED, APART, WINDOW = (40, 40, 200), (10, 10, 50), (8, 8, 48), (16, 16, 56)
WIDTH = (3200, 3200, 640)


def plan():
    ahead, rate, trip = 1.0, 46.6e3, 2.2
    sizes, tasks = {}, {}
    for w, l, h in FLOWS:
        one, two, three = ((axis, l) for axis in ORDER[w][l][h])
        width = COLS[w][h][1] * 2
        whole, back, last = width * (40 if w < 2 else 224), width * (40 if w < 2 else 192), width * WINDOW[w]
        add = 5 / 2 / 1024 / 1900
        for t in range(3):
            on = t < 2
            for k in range(4):
                a = ("a", w, l, h, t, k)
                sizes[a] = (one, whole, 1 + h)
                then = [("a", w, l, h, t + 1, k)] if on else [("b", w, l, h, 0)] if k == 0 else []
                then += [("a", w, l, h + 1, 0, k)] if t == 1 and h + 1 < len(HALVES) else []
                tasks[a] = (a, [], whole * add, then)
                r = ("r", w, l, h, t, k)
                sizes[r] = (one, back, 5 + h)
                tasks[r] = (r, [("q", w, l, h, 2)], 0.05, [("r", w, l, h, t + 1, k)] if on else [])
            b, c, p, q = ((name, w, l, h, t) for name in "bcpq")
            sizes.update({b: (two, whole, 0), c: (three, last, 0), p: (three, last, 0), q: (two, back, 0)})
            tasks[b] = (b, [("a", w, l, h, 2, t + 1)], whole * add, [("b", w, l, h, t + 1)] if on else [("c", w, l, h, 0)])
            tasks[c] = (c, [("b", w, l, h, 2)], last * add, [("c", w, l, h, t + 1)] if on else [])
            tasks[p] = (p, [("step", w, h)], 0.05 if on else 0.4, [("p", w, l, h, t + 1)] if on else [("q", w, l, h, 0), ("r", w, l, h, 0, 0)])
            tasks[q] = (q, [("p", w, l, h, 2)], 0.05, ([("q", w, l, h, t + 1)] if on else []) + [("r", w, l, h, 0, t + 1)])
    for h in HALVES:
        for w in range(3):
            tasks["step", w, h] = (None, [("c", w, l, h, 2) for l in range(2)], 1.5, [("p" if w < 2 else "e", w, l, h, 0) for l in range(2)])
        for l in range(2):
            e = ("e", 2, l, h, 0)
            sizes[e] = ((2, 1), 16 * COLS[2][h][1], 0)
            tasks[e] = (e, [("step", 2, h)], 0.1, [("p", 2, l, h, 0)])
    waiting, free, arrived, done, steps, count = {}, {}, {}, {}, [], 0

    def push(message):
        nonlocal count
        link, _, rank = sizes[message]
        waiting.setdefault(link, []).append((rank, count, message))
        waiting[link].sort()
        count += 1

    for k in range(4):
        for w in range(3):
            for l in range(2):
                push(("a", w, l, 0, 0, k))
    now = 0.0
    while tasks:
        issued = True
        while issued:
            ready = []
            for place, (task, (message, before, _, _)) in enumerate(tasks.items()):
                if (message is None or message in arrived) and all(b in done for b in before):
                    ready.append((max([arrived.get(message, 0.0)] + [done[b] for b in before]), place, task))
            at, _, task = min(ready) if ready else (now, 0, None)
            until, issued = max(now + ahead, at + 1.0), False
            for link in sorted(waiting):
                while waiting[link] and free.get(link, 0.0) < until:
                    message = waiting[link].pop(0)[2]
                    free[link] = max(free.get(link, 0.0), now) + sizes[message][1] / rate
                    arrived[message] = free[link] + trip
                    steps.append(("send", message))
                    issued = True
        _, _, time, then = tasks.pop(task)
        now = max(now, at) + time
        done[task] = now
        steps.append(("task", task))
        for message in then:
            push(message)
    return steps


def ring(p, sign, steps):
    return lax.rem(p + 8 - sign * steps, 4)


def rows8(i, size):
    return pl.ds(pl.multiple_of(i, 8), size)


def over_rows(ref, body):
    if len(ref.shape) == 3:
        lax.fori_loop(0, ref.shape[0], lambda j, _: (body((j,)), 0)[1], 0)
    elif ref.shape[0] == 40:
        lax.fori_loop(0, 5, lambda j, _: (body((rows8(8 * j, 8),)), 0)[1], 0)
    else:
        body((slice(None),))


def add_to(out, a, b):
    def one(i):
        out[i] = (a[i].astype(F32) + b[i].astype(F32)).astype(BF16)

    over_rows(out, one)


LOADS = (6, 5)


def kernel(*refs):
    refs = list(refs)

    def take(n):
        taken = tuple(refs[:n])
        del refs[:n]
        return taken

    terms, weights, ms, vs, outs, mo, vo = (take(3) for _ in range(7))
    r1, r2, r3, held = take(3), take(3), take(3), take(2)
    total, wide, near, mb, vb = take(3), take(3), take(3), take(3), take(3)
    ends, cells, (new, edge) = take(2), take(2), take(2)
    a_send, a_recv, b_send, b_recv, c_send, c_recv, e_send, e_recv = take(8)
    p_send, p_recv, q_send, q_recv, r_send, r_recv = take(6)
    load_sem, in_sem, own_sem, out_sem = take(4)

    me = lax.axis_index("dp")
    at = x, y, z = lax.div(me, 16), lax.rem(lax.div(me, 4), 4), lax.rem(me, 4)

    def towards(axis, sign):
        to = list(at)
        to[axis] = lax.rem(at[axis] + 4 + sign, 4)
        return {"dp": to[0] * 16 + to[1] * 4 + to[2]}

    def cols(w, h):
        return pl.ds(*COLS[w][h])

    def source(w, l, h, block, k):
        a, b, _ = ORDER[w][l][h]
        chunk = ring(at[b], SIGN[l], 1 + k)
        if w < 2:
            i, j = (block, chunk) if a == 0 else (chunk, block)
            return terms[w].at[l, i, j, :, cols(w, h)]
        window = rows8(block * 48, 56)
        return terms[w].at[l, chunk, :, window, cols(w, h)] if b == 0 else terms[w].at[l, :, chunk, window, cols(w, h)]

    def slot(w, h, n):
        n = n % LOADS[w // 2]
        return held[0].at[n, :, pl.ds(0, COLS[w][h][1])] if w < 2 else held[1].at[n, :, :, pl.ds(0, COLS[w][h][1])]

    steps = plan()
    loads = [[task for kind, task in steps if kind == "task" and task[0] == "a" and (task[1] == 2) == down] for down in (False, True)]

    def load(down, n):
        _, w, l, h, t, k = loads[down][n]
        block = ring(at[ORDER[w][l][h][0]], SIGN[l], 2 + t)
        return pltpu.make_async_copy(source(w, l, h, block, k), slot(w, h, n), load_sem.at[down, n % LOADS[down]])

    def part(ref, w, h):
        return ref.at[(slice(None),) * (len(ref.shape) - 1) + (cols(w, h),)]

    def last(w, l, h, t):
        block = ring(at[ORDER[w][l][h][2]], SIGN[l], 2 + t)
        return r2[w].at[l, 2, rows8(block * 8, 16), cols(w, h)] if w < 2 else r2[w].at[l, 2, block, :, cols(w, h)]

    def tiles(block, first):
        return pl.ds(0, 56) if first else rows8(block * 48 + 8, 48)

    def message(name, w, l, h, t, k=0, first=False):
        one, two, three = ORDER[w][l][h]
        s = SIGN[l]
        if name == "a":
            axis, sems = one, (a_send.at[w, l, h, k], a_recv.at[w, l, h, t, k])
            dst = part(r1[w].at[l, t, k], w, h)
            src = source(w, l, h, ring(at[one], s, 1), k) if t == 0 else part(r1[w].at[l, t - 1, k], w, h)
        elif name == "b":
            axis, sems = two, (b_send.at[w, l, h], b_recv.at[w, l, h, t])
            dst = part(r2[w].at[l, t], w, h)
            src = part(r1[w].at[l, 2, 0] if t == 0 else r2[w].at[l, t - 1], w, h)
        elif name == "c":
            axis, sems = three, (c_send.at[w, l, h], c_recv.at[w, l, h, t])
            dst = part(r3[w].at[l, t], w, h)
            src = last(w, l, h, -1) if t == 0 else part(r3[w].at[l, t - 1], w, h)
        elif name == "e":
            axis, s, sems = 2, -1, (e_send.at[l, h], e_recv.at[l, h])
            src, dst = part(new.at[l, pl.ds(0, 8)], w, h), part(edge.at[l], w, h)
        elif name == "p":
            axis, sems = three, (p_send.at[w, l, h], p_recv.at[w, l, h, t])
            block = ring(at[three], s, t)
            if w < 2:
                src = dst = part(ends[w].at[l, block], w, h)
            else:
                i, j = (x, block) if three == 1 else (block, y)
                src = dst = outs[2].at[l, i, j, tiles(z, first), cols(w, h)]
                if t == 0:
                    src = new.at[l, pl.ds(0, 56) if first else pl.ds(8, 48), cols(w, h)]
        elif name == "q":
            axis, sems = two, (q_send.at[w, l, h], q_recv.at[w, l, h, t])
            block = ring(at[two], s, t)
            if w < 2:
                i, j = (x, block) if two == 1 else (block, y)
                src = dst = outs[w].at[l, i, j, :, cols(w, h)]
                if t == 0:
                    src = part(cells[w].at[l], w, h)
            else:
                i, j = (slice(None), block) if two == 1 else (block, slice(None))
                src = dst = outs[2].at[l, i, j, tiles(z, first), cols(w, h)]
        else:
            axis, sems = one, (r_send.at[w, l, h, k], r_recv.at[w, l, h, t, k])
            block, chunk = ring(at[one], s, t), ring(at[two], s, k)
            if w < 2:
                i, j = (block, chunk) if one == 0 else (chunk, block)
                src = dst = outs[w].at[l, i, j, :, cols(w, h)]
                if t == k == 0:
                    src = part(cells[w].at[l], w, h)
            else:
                i, j = (slice(None), chunk) if two == 1 else (chunk, slice(None))
                src = dst = outs[2].at[l, i, j, tiles(block, first), cols(w, h)]
        return pltpu.make_async_remote_copy(
            src_ref=src, dst_ref=dst, send_sem=sems[0], recv_sem=sems[1], device_id=towards(axis, s), device_id_type=MESH
        )

    def each(m, act, coming=False):
        name, w, l, h, t = m[:5]
        if w < 2 or name not in "pqr":
            act(message(*m))
            return
        block = z if name != "r" else ring(z, SIGN[l], t + coming)
        pl.when(block == 0)(lambda: act(message(*m, first=True)))
        pl.when(block != 0)(lambda: act(message(*m)))

    def start(m):
        each(m, lambda copy: copy.start())

    def came(m):
        name, w, l, h, t = m[:5]
        each(m, lambda copy: copy.wait_recv(), coming=True)

    def gone(m):
        each(m, lambda copy: copy.wait_send())

    def inputs():
        for w in range(3):
            yield pltpu.make_async_copy(ms[w], mb[w], in_sem.at[w, 0])
            yield pltpu.make_async_copy(vs[w], vb[w], in_sem.at[w, 1])
            yield pltpu.make_async_copy(weights[w].at[:, x, y, rows8(z * APART[w], WINDOW[w]), :], near[w], in_sem.at[w, 2])

    def own(w, l, h, first=False):
        if w < 2:
            return pltpu.make_async_copy(part(cells[w].at[l], w, h), outs[w].at[l, x, y, :, cols(w, h)], own_sem.at[w, l, h])
        src = new.at[l, pl.ds(0, 56) if first else pl.ds(8, 48), cols(w, h)]
        return pltpu.make_async_copy(src, outs[2].at[l, x, y, tiles(z, first), cols(w, h)], own_sem.at[w, l, h])

    def own_each(w, l, h, act):
        if w < 2:
            act(own(w, l, h))
        else:
            pl.when(z == 0)(lambda: act(own(w, l, h, True)))
            pl.when(z != 0)(lambda: act(own(w, l, h)))

    def optimizer(w, h):
        c = cols(w, h)
        width = COLS[w][h][1]

        def one(r, _):
            row = pl.ds(r + 2 * z, 1)
            g = jnp.concatenate([total[w][l, row, c] for l in range(2)], 0)
            old = jnp.concatenate([wide[w][l, row, c] for l in range(2)], 0)
            m = 0.9 * mb[w][r, :, c] + 0.1 * g
            v = 0.95 * vb[w][r, :, c] + 0.05 * g * g
            step = m * lax.rsqrt(v + 1e-8) + 0.1 * old
            out = old - 0.02 * step
            mb[w][r, :, c] = m
            vb[w][r, :, c] = v
            for l in range(2):
                wide[w][l, row, c] = out[l : l + 1]
            return 0

        lax.fori_loop(0, OWNED[w], one, 0)
        for l in range(2):
            to = ends[w].at[l, z] if w < 2 else new.at[l]
            to[:, c] = wide[w][l, :, c].astype(BF16)

    def join(w, l, h):
        c = cols(w, h)
        row = lax.broadcasted_iota(jnp.int32, (8, COLS[w][h][1]), 0)
        top = [ends[w][l, i, 0:8, c].astype(F32) for i in range(4)]
        low = [ends[w][l, i, 8:16, c].astype(F32) for i in range(4)]
        for i, tile in enumerate([top[0], *(jnp.where(row < 2 * i, low[i - 1], top[i]) for i in (1, 2, 3)), low[3]]):
            cells[w][l, 8 * i : 8 * i + 8, c] = tile.astype(BF16)

    def mend(l, h):
        c = cols(2, h)
        row = lax.broadcasted_iota(jnp.int32, (8, COLS[2][h][1]), 0)
        new[l, 48:56, c] = jnp.where(row < 2 * z + 2, new[l, 48:56, c].astype(F32), edge[l, :, c].astype(F32)).astype(BF16)

    for copy in inputs():
        copy.start()
    for down in range(2):
        for n in range(LOADS[down]):
            load(down, n).start()
    barrier = pltpu.get_barrier_semaphore()
    for axis in range(3):
        for sign in SIGN:
            pl.semaphore_signal(barrier, inc=1, device_id=towards(axis, sign), device_id_type=MESH)
    pl.semaphore_wait(barrier, 6)

    used, begun = [0, 0], False
    flying = {}

    def key(m):
        return (*m[:4], m[5] if len(m) > 5 else 0)

    for kind, task in steps:
        if kind == "send":
            if key(task) in flying:
                gone(flying.pop(key(task)))
            if task[0] == "q" and task[1] == 2 and task[4] == 0:
                own_each(*task[1:4], lambda copy: copy.wait())
            start(task)
            flying[key(task)] = task
            continue
        if not begun:
            for copy in inputs():
                copy.wait()
            for w in range(3):
                for l in range(2):
                    wide[w][l] = near[w][l].astype(F32)
            begun = True
        name, w, *rest = task
        if name == "step":
            optimizer(w, rest[0])
            if rest[0] == len(HALVES) - 1:
                pltpu.make_async_copy(mb[w], mo[w], out_sem.at[w, 0]).start()
                pltpu.make_async_copy(vb[w], vo[w], out_sem.at[w, 1]).start()
            continue
        came(task)
        l, h, t, *k = rest
        if name == "a":
            down = w // 2
            n = used[down]
            used[down] += 1
            load(down, n).wait()
            to = part(r1[w].at[l, t, k[0]], w, h)
            add_to(to, to, slot(w, h, n))
            if n + LOADS[down] < len(loads[down]):
                load(down, n + LOADS[down]).start()
        elif name == "b":
            to = part(r2[w].at[l, t], w, h)
            add_to(to, to, part(r1[w].at[l, 2, t + 1], w, h))
        elif name == "c":
            to = part(r3[w].at[l, t], w, h)
            add_to(to, to, last(w, l, h, t))
            if t == 2:
                total[w][l, :, cols(w, h)] = to[...].astype(F32)
        elif name == "e":
            gone(flying.pop(key(task)))
            mend(l, h)
            own_each(w, l, h, lambda copy: copy.start())
        elif name == "p" and t == 2 and w < 2:
            join(w, l, h)
            own_each(w, l, h, lambda copy: copy.start())
    for task in flying.values():
        gone(task)
    for w, l, h in FLOWS:
        if w < 2:
            own_each(w, l, h, lambda copy: copy.wait())
    for w in range(3):
        pltpu.make_async_copy(mb[w], mo[w], out_sem.at[w, 0]).wait()
        pltpu.make_async_copy(vb[w], vo[w], out_sem.at[w, 1]).wait()


SHAPES = ((2, 4, 4, 40, 3200),) * 2 + ((2, 4, 4, 200, 640),)
MOMENTS = ((10, 2, 3200),) * 2 + ((50, 2, 640),)


def exchanged(*arrays):
    dma, vmem = pltpu.SemaphoreType.DMA, pltpu.VMEM
    flow = len(HALVES)
    cells = ((40, 3200), (40, 3200), (4, 56, 640))
    ring_sems = [dma((3, 2, flow)), dma((3, 2, flow, 3))]
    chunk_sems = [dma((3, 2, flow, 4)), dma((3, 2, flow, 3, 4))]
    windows = [(2, n, width) for n, width in zip(WINDOW, WIDTH, strict=True)]
    return pl.pallas_call(
        kernel,
        out_shape=[jax.ShapeDtypeStruct(s, BF16) for s in SHAPES] + [jax.ShapeDtypeStruct(s, F32) for s in MOMENTS * 2],
        in_specs=[pl.BlockSpec(memory_space=pltpu.HBM)] * 12,
        out_specs=[pl.BlockSpec(memory_space=pl.ANY)] * 9,
        scratch_shapes=[
            *(vmem((2, 3, 4, *c), BF16) for c in cells),
            *(vmem((2, 3, *c), BF16) for c in cells),
            *(vmem((2, 3, *s[1:]), BF16) for s in windows),
            vmem((LOADS[0], 40, COLS[0][0][1]), BF16),
            vmem((LOADS[1], 4, 56, COLS[2][0][1]), BF16),
            *(vmem(s, F32) for s in windows),
            *(vmem(s, F32) for s in windows),
            *(vmem(s, BF16) for s in windows),
            *(vmem(s, F32) for s in MOMENTS * 2),
            *(vmem((2, 4, 16, 3200), BF16),) * 2,
            *(vmem((2, 40, 3200), BF16),) * 2,
            vmem((2, 56, 640), BF16),
            vmem((2, 8, 640), BF16),
            *chunk_sems,
            *ring_sems,
            *ring_sems,
            dma((2, flow)),
            dma((2, flow)),
            *ring_sems,
            *ring_sems,
            *chunk_sems,
            dma((2, max(LOADS))),
            dma((3, 3)),
            dma((3, 2, flow)),
            dma((3, 2)),
        ],
        compiler_params=pltpu.CompilerParams(collective_id=0, has_side_effects=True, vmem_limit_bytes=38 * 2**20),
        name="sum_step_gather",
    )(*arrays)


def put_kernel(*refs):
    ins, outs, sem = refs[:9], refs[9:18], refs[18]
    copies = [pltpu.make_async_copy(a, b, sem.at[i]) for i, (a, b) in enumerate(zip(ins, outs, strict=True))]
    for copy in copies:
        copy.start()
    for copy in copies:
        copy.wait()


def put(arrays):
    return pl.pallas_call(
        put_kernel,
        out_shape=[jax.ShapeDtypeStruct(a.shape, a.dtype) for a in arrays],
        in_specs=[pl.BlockSpec(memory_space=pl.ANY)] * 9,
        out_specs=[pl.BlockSpec(memory_space=pltpu.HBM)] * 9,
        scratch_shapes=[pltpu.SemaphoreType.DMA((9,))],
        compiler_params=pltpu.CompilerParams(vmem_limit_bytes=2**20),
        name="put",
    )(*arrays)


def solution(mesh):
    def step(*arrays):
        terms, weights, m, v = (arrays[i : i + 3] for i in (0, 3, 6, 9))
        cut = [a.reshape(s) for a, s in zip((*terms, *weights), SHAPES * 2, strict=True)]
        moments = [a.transpose(1, 0, 2) for a in (*m, *v)]
        out = put(exchanged(*cut, *moments))
        return (*(o.reshape(w.shape) for o, w in zip(out, weights, strict=False)), *(o.transpose(1, 0, 2) for o in out[3:]))

    all_of, cut = P(None, None, None), P(None, "dp", None)
    return jax.shard_map(
        step,
        mesh=mesh,
        in_specs=(P(("rep", "dp"), None, None, None),) * 3 + (all_of,) * 3 + (cut,) * 6,
        out_specs=(P("rep", None, None),) * 3 + (P("rep", "dp", None),) * 6,
        check_vma=False,
    )
```

```python
import jax
import jax.numpy as jnp
from jax import lax
from jax.experimental import pallas as pl
from jax.experimental.pallas import tpu as pltpu
from jax.sharding import PartitionSpec as P

BF16, F32 = jnp.bfloat16, jnp.float32
LOGICAL = pl.DeviceIdType.LOGICAL
SIGN = (1, -1)
COLS = (((0, 1664), (1664, 1536)),) * 2 + (((0, 384), (384, 256)),)
HALVES = LAYERS = (0, 1)
WEIGHTS = AXES = HOPS = (0, 1, 2)
CHUNKS = (0, 1, 2, 3)
DOWN = 2
ALL = slice(None)
IN_HBM, IN_VMEM, ANYWHERE = (pl.BlockSpec(memory_space=space) for space in (pltpu.HBM, pltpu.VMEM, pl.ANY))
XYZ, YXZ, ZXY, ZYX = (0, 1, 2), (1, 0, 2), (2, 0, 1), (2, 1, 0)
ORDER = (((XYZ, XYZ),) * 2, ((YXZ, YXZ),) * 2, ((ZXY, ZYX), (ZYX, ZXY)))
FLOWS = tuple((w, l, h) for h in HALVES for w in WEIGHTS for l in LAYERS)
CELL, OWNED, APART, WINDOW = (40, 40, 200), (10, 10, 50), (8, 8, 48), (16, 16, 56)
WIDTH = (3200, 3200, 640)


def plan():
    ahead, rate, trip = 1.0, 46.6e3, 2.2
    sizes, tasks = {}, {}
    for w, l, h in FLOWS:
        one, two, three = ((axis, l) for axis in ORDER[w][l][h])
        width = COLS[w][h][1] * 2
        whole, back, last = width * (40 if w < DOWN else 224), width * (40 if w < DOWN else 192), width * WINDOW[w]
        add = 5 / 2 / 1024 / 1900
        for t in HOPS:
            on = t < 2
            for k in CHUNKS:
                a = ("a", w, l, h, t, k)
                sizes[a] = (one, whole, 1 + h)
                then = [("a", w, l, h, t + 1, k)] if on else [("b", w, l, h, 0)] if k == 0 else []
                then += [("a", w, l, h + 1, 0, k)] if t == 1 and h + 1 < len(HALVES) else []
                tasks[a] = (a, [], whole * add, then)
                r = ("r", w, l, h, t, k)
                sizes[r] = (one, back, 5 + h)
                tasks[r] = (r, [("q", w, l, h, 2)], 0.05, [("r", w, l, h, t + 1, k)] if on else [])
            b, c, p, q = ((name, w, l, h, t) for name in "bcpq")
            sizes.update({b: (two, whole, 0), c: (three, last, 0), p: (three, last, 0), q: (two, back, 0)})
            tasks[b] = (b, [("a", w, l, h, 2, t + 1)], whole * add, [("b", w, l, h, t + 1)] if on else [("c", w, l, h, 0)])
            tasks[c] = (c, [("b", w, l, h, 2)], last * add, [("c", w, l, h, t + 1)] if on else [])
            tasks[p] = (p, [("step", w, h)], 0.05 if on else 0.4, [("p", w, l, h, t + 1)] if on else [("q", w, l, h, 0), ("r", w, l, h, 0, 0)])
            tasks[q] = (q, [("p", w, l, h, 2)], 0.05, ([("q", w, l, h, t + 1)] if on else []) + [("r", w, l, h, 0, t + 1)])
    for h in HALVES:
        for w in WEIGHTS:
            tasks["step", w, h] = (None, [("c", w, l, h, 2) for l in LAYERS], 1.5, [("p" if w < DOWN else "e", w, l, h, 0) for l in LAYERS])
        for l in LAYERS:
            e = ("e", 2, l, h, 0)
            sizes[e] = ((2, 1), 16 * COLS[2][h][1], 0)
            tasks[e] = (e, [("step", 2, h)], 0.1, [("p", 2, l, h, 0)])
    waiting, free, arrived, done, steps, count = {}, {}, {}, {}, [], 0

    def push(message):
        nonlocal count
        link, _, rank = sizes[message]
        waiting.setdefault(link, []).append((rank, count, message))
        waiting[link].sort()
        count += 1

    for k in CHUNKS:
        for w in WEIGHTS:
            for l in LAYERS:
                push(("a", w, l, 0, 0, k))
    now = 0.0
    while tasks:
        issued = True
        while issued:
            ready = []
            for place, (task, (message, before, _, _)) in enumerate(tasks.items()):
                if (message is None or message in arrived) and all(b in done for b in before):
                    ready.append((max([arrived.get(message, 0.0)] + [done[b] for b in before]), place, task))
            at, _, task = min(ready) if ready else (now, 0, None)
            until, issued = max(now + ahead, at + 1.0), False
            for link in sorted(waiting):
                while waiting[link] and free.get(link, 0.0) < until:
                    message = waiting[link].pop(0)[2]
                    free[link] = max(free.get(link, 0.0), now) + sizes[message][1] / rate
                    arrived[message] = free[link] + trip
                    steps.append(("send", message))
                    issued = True
        _, _, time, then = tasks.pop(task)
        now = max(now, at) + time
        done[task] = now
        steps.append(("task", task))
        for message in then:
            push(message)
    return steps


def rows8(i, size):
    return pl.ds(pl.multiple_of(i, 8), size)


def over_rows(ref, body):
    if len(ref.shape) == 3:
        lax.fori_loop(0, ref.shape[0], lambda j, _: (body((j,)), 0)[1], 0)
    elif ref.shape[0] == 40:
        lax.fori_loop(0, 5, lambda j, _: (body((rows8(8 * j, 8),)), 0)[1], 0)
    else:
        body((ALL,))


def either(first, yes, no):
    def call(act):
        act()

    lax.cond(first, lambda: call(yes), lambda: call(no))


def add_to(out, a, b):
    def one(i):
        out[i] = (a[i].astype(F32) + b[i].astype(F32)).astype(BF16)

    over_rows(out, one)


LOADS = (8, 6)


def kernel(*refs):
    refs = list(refs)

    def take(n):
        taken = tuple(refs[:n])
        del refs[:n]
        return taken

    def halved(n):
        return [take(len(HALVES)) for _ in range(n)]

    terms, weights, ms, vs = (take(3) for _ in range(4))
    outs, mo, vo = halved(3), take(3), take(3)
    r1, r2, r3, held = halved(3), halved(3), halved(3), take(2)
    total, wide, near = take(2), take(2), take(3)
    ends, cells, (new, edge) = halved(2), halved(2), halved(2)
    a_send, a_recv, b_send, b_recv, c_send, c_recv, e_send, e_recv = take(8)
    p_send, p_recv, q_send, q_recv, r_send, r_recv = take(6)
    load_sem, in_sem, own_sem = take(3)

    me = lax.axis_index("dp")
    at = x, y, z = lax.div(me, 16), lax.rem(lax.div(me, 4), 4), lax.rem(me, 4)

    places = [[at[axis]] + [lax.rem(at[axis] + n, 4) for n in (1, 2, 3)] for axis in AXES]
    eights, windows, bands = ([[f(p) for p in places[axis]] for axis in AXES] for f in (lambda p: 8 * p, lambda p: 48 * p, lambda p: 48 * p + 8))
    firsts = [p == 0 for p in places[2]]
    next_to = {}
    for axis in AXES:
        for sign in SIGN:
            to = list(at)
            to[axis] = places[axis][sign % 4]
            next_to[axis, sign] = lax.axis_index("rep") * 64 + to[0] * 16 + to[1] * 4 + to[2]

    def towards(axis, sign):
        return next_to[axis, sign]

    def ring(axis, sign, steps, of=places):
        return of[axis][-sign * steps % 4]

    def number(w, l, h):
        return (w * 2 + l) * len(HALVES) + h

    def cols(w, h):
        return pl.ds(*COLS[w][h])

    def source(w, l, h, steps, k):
        a, b, _ = ORDER[w][l][h]
        chunk = ring(b, SIGN[l], 1 + k)
        if w < DOWN:
            block = ring(a, SIGN[l], steps)
            i, j = (block, chunk) if a == 0 else (chunk, block)
            return terms[w].at[l, i, j, :, cols(w, h)]
        window = rows8(ring(a, SIGN[l], steps, windows), 56)
        return terms[w].at[l, chunk, :, window, cols(w, h)] if b == 0 else terms[w].at[l, :, chunk, window, cols(w, h)]

    def slot(w, h, n):
        n = n % LOADS[w // 2]
        return held[0].at[n, :, pl.ds(0, COLS[w][h][1])] if w < DOWN else held[1].at[n, :, :, pl.ds(0, COLS[w][h][1])]

    steps = plan()
    loads = [[task for kind, task in steps if kind == "task" and task[0] == "a" and (task[1] == DOWN) == down] for down in (False, True)]

    def load(down, n):
        _, w, l, h, t, k = loads[down][n]
        return pltpu.make_async_copy(source(w, l, h, 2 + t, k), slot(w, h, n), load_sem.at[down * LOADS[0] + n % LOADS[down]])

    def spot(refs, w, l, h, t, k=None):
        return refs[w][h].at[l * 3 + t if k is None else l * 12 + t * 4 + k]

    def last(w, l, h, t):
        axis = ORDER[w][l][h][2]
        if w < DOWN:
            return r2[w][h].at[l * 3 + 2, rows8(ring(axis, SIGN[l], 2 + t, eights), 16)]
        return r2[w][h].at[l * 3 + 2, ring(axis, SIGN[l], 2 + t)]

    def tiles(steps, first):
        return pl.ds(0, 56) if first else rows8(bands[2][-steps % 4], 48)

    def message(name, w, l, h, t, k=0, first=False):
        one, two, three = ORDER[w][l][h]
        s, n = SIGN[l], number(w, l, h)
        if name == "a":
            axis, sems = one, (a_send.at[n * 4 + k], a_recv.at[n * 12 + t * 4 + k])
            dst = spot(r1, w, l, h, t, k)
            src = source(w, l, h, 1, k) if t == 0 else spot(r1, w, l, h, t - 1, k)
        elif name == "b":
            axis, sems = two, (b_send.at[n], b_recv.at[n * 3 + t])
            dst = spot(r2, w, l, h, t)
            src = spot(r1, w, l, h, 2, 0) if t == 0 else spot(r2, w, l, h, t - 1)
        elif name == "c":
            axis, sems = three, (c_send.at[n], c_recv.at[n * 3 + t])
            dst = spot(r3, w, l, h, t)
            src = last(w, l, h, -1) if t == 0 else spot(r3, w, l, h, t - 1)
        elif name == "e":
            axis, s, sems = 2, -1, (e_send.at[n - 4 * len(HALVES)], e_recv.at[n - 4 * len(HALVES)])
            src, dst = new[h].at[l, pl.ds(0, 8)], edge[h].at[l]
        elif name == "p":
            axis, sems = three, (p_send.at[n], p_recv.at[n * 3 + t])
            block = ring(three, s, t)
            if w < DOWN:
                src = dst = ends[w][h].at[l, block]
            else:
                i, j = (x, block) if three == 1 else (block, y)
                src = dst = outs[DOWN][h].at[l, i, j, tiles(0, first)]
                if t == 0:
                    src = new[h].at[l, pl.ds(0, 56) if first else pl.ds(8, 48)]
        elif name == "q":
            axis, sems = two, (q_send.at[n], q_recv.at[n * 3 + t])
            block = ring(two, s, t)
            if w < DOWN:
                i, j = (x, block) if two == 1 else (block, y)
                src = dst = outs[w][h].at[l, i, j]
                if t == 0:
                    src = cells[w][h].at[l]
            else:
                i, j = (ALL, block) if two == 1 else (block, ALL)
                src = dst = outs[DOWN][h].at[l, i, j, tiles(0, first)]
        else:
            axis, sems = one, (r_send.at[n * 4 + k], r_recv.at[n * 12 + t * 4 + k])
            block, chunk = ring(one, s, t), ring(two, s, k)
            if w < DOWN:
                i, j = (block, chunk) if one == 0 else (chunk, block)
                src = dst = outs[w][h].at[l, i, j]
                if t == k == 0:
                    src = cells[w][h].at[l]
            else:
                i, j = (ALL, chunk) if two == 1 else (chunk, ALL)
                src = dst = outs[DOWN][h].at[l, i, j, tiles(s * t, first)]
        return pltpu.make_async_remote_copy(
            src_ref=src, dst_ref=dst, send_sem=sems[0], recv_sem=sems[1], device_id=towards(axis, s), device_id_type=LOGICAL
        )

    def each(m, act, coming=False):
        name, w, l, h, t = m[:5]
        if w < DOWN or name not in "pqr":
            act(message(*m))
            return
        first = firsts[0] if name != "r" else ring(0, SIGN[l], t + coming, [firsts])
        either(first, lambda: act(message(*m, first=True)), lambda: act(message(*m)))

    def start(m):
        each(m, lambda copy: copy.start())

    def came(m):
        name, w, l, h, t = m[:5]
        each(m, lambda copy: copy.wait_recv(), coming=True)

    def gone(m):
        each(m, lambda copy: copy.wait_send())

    def inputs():
        for w in WEIGHTS:
            yield pltpu.make_async_copy(weights[w].at[:, x, y, rows8(z * APART[w], WINDOW[w]), :], near[w], in_sem.at[w])

    def own(w, l, h, first=False):
        if w < DOWN:
            return pltpu.make_async_copy(cells[w][h].at[l], outs[w][h].at[l, x, y], own_sem.at[number(w, l, h)])
        src = new[h].at[l, pl.ds(0, 56) if first else pl.ds(8, 48)]
        return pltpu.make_async_copy(src, outs[DOWN][h].at[l, x, y, tiles(0, first)], own_sem.at[number(w, l, h)])

    def own_each(w, l, h, act):
        if w < DOWN:
            act(own(w, l, h))
        else:
            either(firsts[0], lambda: act(own(w, l, h, True)), lambda: act(own(w, l, h)))

    def optimizer(w, h):
        c = cols(w, h)

        grad, weight = (ref.at[:, :, pl.ds(0, COLS[w][h][1])] for ref in (total[w // 2], wide[w // 2]))
        for l in LAYERS:
            grad[l] = r3[w][h][l * 3 + 2].astype(F32)
            weight[l] = near[w][l, :, c].astype(F32)

        def one(r, _):
            row = pl.ds(r + 2 * z, 1)
            g = jnp.concatenate([grad[l, row, :] for l in LAYERS], 0)
            old = jnp.concatenate([weight[l, row, :] for l in LAYERS], 0)
            m = 0.9 * ms[w][r, :, c] + 0.1 * g
            v = 0.95 * vs[w][r, :, c] + 0.05 * g * g
            step = m * lax.rsqrt(v + 1e-8) + 0.1 * old
            out = old - 0.02 * step
            mo[w][r, :, c] = m
            vo[w][r, :, c] = v
            for l in LAYERS:
                weight[l, row, :] = out[l : l + 1]
            return 0

        lax.fori_loop(0, OWNED[w], one, 0)
        for l in LAYERS:
            to = ends[w][h].at[l, z] if w < DOWN else new[h].at[l]
            to[...] = weight[l].astype(BF16)

    def join(w, l, h):
        row = lax.broadcasted_iota(jnp.int32, (8, COLS[w][h][1]), 0)
        top = [ends[w][h][l, i, 0:8].astype(F32) for i in range(4)]
        low = [ends[w][h][l, i, 8:16].astype(F32) for i in range(4)]
        for i, tile in enumerate([top[0], *(jnp.where(row < DOWN * i, low[i - 1], top[i]) for i in (1, 2, 3)), low[3]]):
            cells[w][h][l, 8 * i : 8 * i + 8] = tile.astype(BF16)

    def mend(l, h):
        row = lax.broadcasted_iota(jnp.int32, (8, COLS[2][h][1]), 0)
        new[h][l, 48:56] = jnp.where(row < DOWN * z + 2, new[h][l, 48:56].astype(F32), edge[h][l].astype(F32)).astype(BF16)

    for copy in inputs():
        copy.start()
    for down in range(2):
        for n in range(LOADS[down]):
            load(down, n).start()
    barrier = pltpu.get_barrier_semaphore()
    for axis in AXES:
        for sign in SIGN:
            pl.semaphore_signal(barrier, inc=1, device_id=towards(axis, sign), device_id_type=LOGICAL)
    pl.semaphore_wait(barrier, 6)

    used, begun = [0, 0], False
    flying, staying = {}, {f for f in FLOWS if f[0] == 2}

    def key(m):
        return (*m[:4], m[5] if len(m) > 5 else 0)

    for kind, task in steps:
        if kind == "send":
            if key(task) in flying:
                gone(flying.pop(key(task)))
            if task[0] in "qr" and task[1] == DOWN and task[1:4] in staying:
                staying.remove(task[1:4])
                own_each(*task[1:4], lambda copy: copy.wait())
            start(task)
            flying[key(task)] = task
            continue
        if not begun:
            for copy in inputs():
                copy.wait()
            begun = True
        name, w, *rest = task
        if name == "step":
            optimizer(w, rest[0])
            continue
        came(task)
        l, h, t, *k = rest
        if name == "a":
            down = w // 2
            n = used[down]
            used[down] += 1
            load(down, n).wait()
            to = spot(r1, w, l, h, t, k[0])
            add_to(to, to, slot(w, h, n))
            if n + LOADS[down] < len(loads[down]):
                load(down, n + LOADS[down]).start()
        elif name == "b":
            to = spot(r2, w, l, h, t)
            add_to(to, to, spot(r1, w, l, h, 2, t + 1))
        elif name == "c":
            to = spot(r3, w, l, h, t)
            add_to(to, to, last(w, l, h, t))
        elif name == "e":
            gone(flying.pop(key(task)))
            mend(l, h)
            own_each(w, l, h, lambda copy: copy.start())
        elif name == "p" and t == 2 and w < DOWN:
            join(w, l, h)
            own_each(w, l, h, lambda copy: copy.start())
    for task in flying.values():
        gone(task)
    for w, l, h in FLOWS:
        if w < DOWN:
            own_each(w, l, h, lambda copy: copy.wait())


SHAPES = ((2, 4, 4, 40, 3200),) * 2 + ((2, 4, 4, 200, 640),)
MOMENTS = ((10, 2, 3200),) * 2 + ((50, 2, 640),)


def exchanged(*arrays):
    dma, vmem = pltpu.SemaphoreType.DMA, pltpu.VMEM
    flow = len(HALVES)
    ring_sems = [dma((6 * flow,)), dma((18 * flow,))]
    chunk_sems = [dma((24 * flow,)), dma((72 * flow,))]

    def halved(weights, shape, dtype=BF16):
        return [vmem((*shape(w), COLS[w][h][1]), dtype) for w in weights for h in HALVES]

    everything, wide, down = WEIGHTS, WEIGHTS[:DOWN], WEIGHTS[DOWN:]
    results = [jax.ShapeDtypeStruct((*SHAPES[w][:4], COLS[w][h][1]), BF16) for w in everything for h in HALVES]
    return pl.pallas_call(
        kernel,
        out_shape=results + [jax.ShapeDtypeStruct(s, F32) for s in MOMENTS * 2],
        in_specs=[IN_HBM] * 6 + [IN_VMEM] * 6,
        out_specs=[ANYWHERE] * (3 * flow) + [IN_VMEM] * 6,
        scratch_shapes=[
            *halved(everything, lambda w: (24, *((40,) if w < DOWN else (4, 56)))),
            *halved(everything, lambda w: (6, *((40,) if w < DOWN else (4, 56)))),
            *halved(everything, lambda w: (6, WINDOW[w])),
            vmem((LOADS[0], 40, COLS[0][0][1]), BF16),
            vmem((LOADS[1], 4, 56, COLS[2][0][1]), BF16),
            *(vmem((2, WINDOW[w], COLS[w][0][1]), F32) for w in (0, 2)),
            *(vmem((2, WINDOW[w], COLS[w][0][1]), F32) for w in (0, 2)),
            *(vmem((2, n, width), BF16) for n, width in zip(WINDOW, WIDTH, strict=True)),
            *halved(wide, lambda w: (2, 4, 16)),
            *halved(wide, lambda w: (2, 40)),
            *halved(down, lambda w: (2, 56)),
            *halved(down, lambda w: (2, 8)),
            *chunk_sems,
            *ring_sems,
            *ring_sems,
            dma((2 * flow,)),
            dma((2 * flow,)),
            *ring_sems,
            *ring_sems,
            *chunk_sems,
            dma((sum(LOADS),)),
            dma((3,)),
            dma((6 * flow,)),
        ],
        compiler_params=pltpu.CompilerParams(collective_id=0, has_side_effects=True, vmem_limit_bytes=31 * 2**20),
        name="sum_step_gather",
    )(*arrays)


def put_kernel(*refs):
    n = len(HALVES)
    ins, outs, sem = refs[: 3 * n + 6], refs[3 * n + 6 : -1], refs[-1]
    pairs = [(ins[w * n + h], outs[w].at[:, :, :, :, pl.ds(*COLS[w][h])]) for w in WEIGHTS for h in HALVES]
    pairs += zip(ins[3 * n :], outs[3:], strict=True)
    copies = [pltpu.make_async_copy(a, b, sem.at[i]) for i, (a, b) in enumerate(pairs)]
    for copy in copies:
        copy.start()
    for copy in copies:
        copy.wait()


def put(arrays):
    return pl.pallas_call(
        put_kernel,
        out_shape=[jax.ShapeDtypeStruct(s, BF16) for s in SHAPES] + [jax.ShapeDtypeStruct(s, F32) for s in MOMENTS * 2],
        in_specs=[ANYWHERE] * len(arrays),
        out_specs=[IN_HBM] * 9,
        scratch_shapes=[pltpu.SemaphoreType.DMA((len(arrays),))],
        compiler_params=pltpu.CompilerParams(vmem_limit_bytes=2**20),
        name="put",
    )(*arrays)


def solution(mesh):
    def step(*arrays):
        terms, weights, m, v = (arrays[i : i + 3] for i in (0, 3, 6, 9))
        cut = [a.reshape(s) for a, s in zip((*terms, *weights), SHAPES * 2, strict=True)]
        moments = [a.transpose(1, 0, 2) for a in (*m, *v)]
        out = put(exchanged(*cut, *moments))
        return (*(o.reshape(w.shape) for o, w in zip(out, weights, strict=False)), *(o.transpose(1, 0, 2) for o in out[3:]))

    all_of, cut = P(None, None, None), P(None, "dp", None)
    return jax.shard_map(
        step,
        mesh=mesh,
        in_specs=(P(("rep", "dp"), None, None, None),) * 3 + (all_of,) * 3 + (cut,) * 6,
        out_specs=(P("rep", None, None),) * 3 + (P("rep", "dp", None),) * 6,
        check_vma=False,
    )
```

```python
import jax
import jax.numpy as jnp
from jax import lax
from jax.experimental import pallas as pl
from jax.experimental.pallas import tpu as pltpu
from jax.sharding import PartitionSpec as P

BF16, F32 = jnp.bfloat16, jnp.float32
LOGICAL = pl.DeviceIdType.LOGICAL
SIGN = (1, -1)
COLS = (((0, 1664), (1664, 1536)),) * 2 + (((0, 384), (384, 256)),)
HALVES = LAYERS = (0, 1)
WEIGHTS = AXES = HOPS = (0, 1, 2)
CHUNKS = (0, 1, 2, 3)
DOWN = 2
ALL = slice(None)
IN_HBM, IN_VMEM, ANYWHERE = (pl.BlockSpec(memory_space=space) for space in (pltpu.HBM, pltpu.VMEM, pl.ANY))
XYZ, YXZ, ZXY, ZYX = (0, 1, 2), (1, 0, 2), (2, 0, 1), (2, 1, 0)
ORDER = (((XYZ, XYZ),) * 2, ((YXZ, YXZ),) * 2, ((ZXY, ZYX), (ZYX, ZXY)))
FLOWS = tuple((w, l, h) for h in HALVES for w in WEIGHTS for l in LAYERS)
CELL, OWNED, APART, WINDOW = (40, 40, 200), (10, 10, 50), (8, 8, 48), (16, 16, 56)
WIDTH = (3200, 3200, 640)


def plan():
    ahead, rate, trip = 1.0, 46.6e3, 3.0
    sizes, tasks = {}, {}
    for w, l, h in FLOWS:
        one, two, three = ((axis, l) for axis in ORDER[w][l][h])
        width = COLS[w][h][1] * 2
        whole, back, last = width * (40 if w < DOWN else 224), width * (40 if w < DOWN else 192), width * WINDOW[w]
        add = 5 / 2 / 1024 / 1900
        for t in HOPS:
            on = t < 2
            for k in CHUNKS:
                a = ("a", w, l, h, t, k)
                sizes[a] = (one, whole, 1 + h)
                then = [("a", w, l, h, t + 1, k)] if on else [("b", w, l, h, 0)] if k == 0 else []
                then += [("a", w, l, h + 1, 0, k)] if t == 1 and h + 1 < len(HALVES) else []
                tasks[a] = (a, [], whole * add, then)
                r = ("r", w, l, h, t, k)
                sizes[r] = (one, back, 5 + h)
                tasks[r] = (r, [("q", w, l, h, 2)], 0.05, [("r", w, l, h, t + 1, k)] if on else [])
            b, c, p, q = ((name, w, l, h, t) for name in "bcpq")
            sizes.update({b: (two, whole, 0), c: (three, last, 0), p: (three, last, 0), q: (two, back, 0)})
            tasks[b] = (b, [("a", w, l, h, 2, t + 1)], whole * add, [("b", w, l, h, t + 1)] if on else [("c", w, l, h, 0)])
            tasks[c] = (c, [("b", w, l, h, 2)], last * add, [("c", w, l, h, t + 1)] if on else [])
            tasks[p] = (p, [("step", w, h)], 0.05 if on else 0.4, [("p", w, l, h, t + 1)] if on else [("q", w, l, h, 0), ("r", w, l, h, 0, 0)])
            tasks[q] = (q, [("p", w, l, h, 2)], 0.05, ([("q", w, l, h, t + 1)] if on else []) + [("r", w, l, h, 0, t + 1)])
    for h in HALVES:
        for w in WEIGHTS:
            tasks["step", w, h] = (None, [("c", w, l, h, 2) for l in LAYERS], 1.5, [("p" if w < DOWN else "e", w, l, h, 0) for l in LAYERS])
        for l in LAYERS:
            e = ("e", 2, l, h, 0)
            sizes[e] = ((2, 1), 16 * COLS[2][h][1], 0)
            tasks[e] = (e, [("step", 2, h)], 0.1, [("p", 2, l, h, 0)])
    waiting, free, arrived, done, steps, count = {}, {}, {}, {}, [], 0

    def push(message):
        nonlocal count
        link, _, rank = sizes[message]
        waiting.setdefault(link, []).append((rank, count, message))
        waiting[link].sort()
        count += 1

    for k in CHUNKS:
        for w in WEIGHTS:
            for l in LAYERS:
                push(("a", w, l, 0, 0, k))
    now = 0.0
    while tasks:
        issued = True
        while issued:
            ready = []
            for place, (task, (message, before, _, _)) in enumerate(tasks.items()):
                if (message is None or message in arrived) and all(b in done for b in before):
                    ready.append((max([arrived.get(message, 0.0)] + [done[b] for b in before]), place, task))
            at, _, task = min(ready) if ready else (now, 0, None)
            until, issued = max(now + ahead, at + 1.0), False
            for link in sorted(waiting):
                while waiting[link] and free.get(link, 0.0) < until:
                    message = waiting[link].pop(0)[2]
                    free[link] = max(free.get(link, 0.0), now) + sizes[message][1] / rate
                    arrived[message] = free[link] + trip
                    steps.append(("send", message))
                    issued = True
        _, _, time, then = tasks.pop(task)
        now = max(now, at) + time
        done[task] = now
        steps.append(("task", task))
        for message in then:
            push(message)
    return steps


def rows8(i, size):
    return pl.ds(pl.multiple_of(i, 8), size)


def over_rows(ref, body):
    if len(ref.shape) == 3:
        lax.fori_loop(0, ref.shape[0], lambda j, _: (body((j,)), 0)[1], 0)
    elif ref.shape[0] == 40:
        lax.fori_loop(0, 5, lambda j, _: (body((rows8(8 * j, 8),)), 0)[1], 0)
    else:
        body((ALL,))


def either(first, yes, no):
    def call(act):
        act()

    lax.cond(first, lambda: call(yes), lambda: call(no))


def add_to(out, a, b):
    def one(i):
        out[i] = (a[i].astype(F32) + b[i].astype(F32)).astype(BF16)

    over_rows(out, one)


LOADS = (8, 6)


def kernel(*refs):
    refs = list(refs)

    def take(n):
        taken = tuple(refs[:n])
        del refs[:n]
        return taken

    def halved(n):
        return [take(len(HALVES)) for _ in range(n)]

    terms, weights, ms, vs = (take(3) for _ in range(4))
    outs, mo, vo = halved(3), take(3), take(3)
    r1, r2, r3, held = halved(3), halved(3), halved(3), take(2)
    total, wide, near, mb, vb = take(2), take(2), take(3), take(3), take(3)
    ends, cells, (new, edge) = halved(2), halved(2), halved(2)
    a_send, a_recv, b_send, b_recv, c_send, c_recv, e_send, e_recv = take(8)
    p_send, p_recv, q_send, q_recv, r_send, r_recv = take(6)
    load_sem, in_sem, own_sem = take(3)

    me = lax.axis_index("dp")
    at = x, y, z = lax.div(me, 16), lax.rem(lax.div(me, 4), 4), lax.rem(me, 4)

    places = [[at[axis]] + [lax.rem(at[axis] + n, 4) for n in (1, 2, 3)] for axis in AXES]
    eights, windows, bands = ([[f(p) for p in places[axis]] for axis in AXES] for f in (lambda p: 8 * p, lambda p: 48 * p, lambda p: 48 * p + 8))
    firsts = [p == 0 for p in places[2]]
    next_to = {}
    for axis in AXES:
        for sign in SIGN:
            to = list(at)
            to[axis] = places[axis][sign % 4]
            next_to[axis, sign] = lax.axis_index("rep") * 64 + to[0] * 16 + to[1] * 4 + to[2]

    def towards(axis, sign):
        return next_to[axis, sign]

    def ring(axis, sign, steps, of=places):
        return of[axis][-sign * steps % 4]

    def number(w, l, h):
        return (w * 2 + l) * len(HALVES) + h

    def cols(w, h):
        return pl.ds(*COLS[w][h])

    def source(w, l, h, steps, k):
        a, b, _ = ORDER[w][l][h]
        chunk = ring(b, SIGN[l], 1 + k)
        if w < DOWN:
            block = ring(a, SIGN[l], steps)
            i, j = (block, chunk) if a == 0 else (chunk, block)
            return terms[w].at[l, i, j, :, cols(w, h)]
        window = rows8(ring(a, SIGN[l], steps, windows), 56)
        return terms[w].at[l, chunk, :, window, cols(w, h)] if b == 0 else terms[w].at[l, :, chunk, window, cols(w, h)]

    def slot(w, h, n):
        n = n % LOADS[w // 2]
        return held[0].at[n, :, pl.ds(0, COLS[w][h][1])] if w < DOWN else held[1].at[n, :, :, pl.ds(0, COLS[w][h][1])]

    steps = plan()
    loads = [[task for kind, task in steps if kind == "task" and task[0] == "a" and (task[1] == DOWN) == down] for down in (False, True)]

    def load(down, n):
        _, w, l, h, t, k = loads[down][n]
        return pltpu.make_async_copy(source(w, l, h, 2 + t, k), slot(w, h, n), load_sem.at[down * LOADS[0] + n % LOADS[down]])

    def spot(refs, w, l, h, t, k=None):
        return refs[w][h].at[l * 3 + t if k is None else l * 12 + t * 4 + k]

    def last(w, l, h, t):
        axis = ORDER[w][l][h][2]
        if w < DOWN:
            return r2[w][h].at[l * 3 + 2, rows8(ring(axis, SIGN[l], 2 + t, eights), 16)]
        return r2[w][h].at[l * 3 + 2, ring(axis, SIGN[l], 2 + t)]

    def tiles(steps, first):
        return pl.ds(0, 56) if first else rows8(bands[2][-steps % 4], 48)

    def message(name, w, l, h, t, k=0, first=False):
        one, two, three = ORDER[w][l][h]
        s, n = SIGN[l], number(w, l, h)
        if name == "a":
            axis, sems = one, (a_send.at[n * 4 + k], a_recv.at[n * 12 + t * 4 + k])
            dst = spot(r1, w, l, h, t, k)
            src = source(w, l, h, 1, k) if t == 0 else spot(r1, w, l, h, t - 1, k)
        elif name == "b":
            axis, sems = two, (b_send.at[n], b_recv.at[n * 3 + t])
            dst = spot(r2, w, l, h, t)
            src = spot(r1, w, l, h, 2, 0) if t == 0 else spot(r2, w, l, h, t - 1)
        elif name == "c":
            axis, sems = three, (c_send.at[n], c_recv.at[n * 3 + t])
            dst = spot(r3, w, l, h, t)
            src = last(w, l, h, -1) if t == 0 else spot(r3, w, l, h, t - 1)
        elif name == "e":
            axis, s, sems = 2, -1, (e_send.at[n - 4 * len(HALVES)], e_recv.at[n - 4 * len(HALVES)])
            src, dst = new[h].at[l, pl.ds(0, 8)], edge[h].at[l]
        elif name == "p":
            axis, sems = three, (p_send.at[n], p_recv.at[n * 3 + t])
            block = ring(three, s, t)
            if w < DOWN:
                src = dst = ends[w][h].at[l, block]
            else:
                i, j = (x, block) if three == 1 else (block, y)
                src = dst = outs[DOWN][h].at[l, i, j, tiles(0, first)]
                if t == 0:
                    src = new[h].at[l, pl.ds(0, 56) if first else pl.ds(8, 48)]
        elif name == "q":
            axis, sems = two, (q_send.at[n], q_recv.at[n * 3 + t])
            block = ring(two, s, t)
            if w < DOWN:
                i, j = (x, block) if two == 1 else (block, y)
                src = dst = outs[w][h].at[l, i, j]
                if t == 0:
                    src = cells[w][h].at[l]
            else:
                i, j = (ALL, block) if two == 1 else (block, ALL)
                src = dst = outs[DOWN][h].at[l, i, j, tiles(0, first)]
        else:
            axis, sems = one, (r_send.at[n * 4 + k], r_recv.at[n * 12 + t * 4 + k])
            block, chunk = ring(one, s, t), ring(two, s, k)
            if w < DOWN:
                i, j = (block, chunk) if one == 0 else (chunk, block)
                src = dst = outs[w][h].at[l, i, j]
                if t == k == 0:
                    src = cells[w][h].at[l]
            else:
                i, j = (ALL, chunk) if two == 1 else (chunk, ALL)
                src = dst = outs[DOWN][h].at[l, i, j, tiles(s * t, first)]
        return pltpu.make_async_remote_copy(
            src_ref=src, dst_ref=dst, send_sem=sems[0], recv_sem=sems[1], device_id=towards(axis, s), device_id_type=LOGICAL
        )

    def each(m, act, coming=False):
        name, w, l, h, t = m[:5]
        if w < DOWN or name not in "pqr":
            act(message(*m))
            return
        first = firsts[0] if name != "r" else ring(0, SIGN[l], t + coming, [firsts])
        either(first, lambda: act(message(*m, first=True)), lambda: act(message(*m)))

    def start(m):
        each(m, lambda copy: copy.start())

    def came(m):
        name, w, l, h, t = m[:5]
        each(m, lambda copy: copy.wait_recv(), coming=True)

    def gone(m):
        each(m, lambda copy: copy.wait_send())

    def inputs():
        for w in WEIGHTS:
            yield pltpu.make_async_copy(weights[w].at[:, x, y, rows8(z * APART[w], WINDOW[w]), :], near[w], in_sem.at[w])
            yield pltpu.make_async_copy(ms[w], mb[w], in_sem.at[w + 3])
            yield pltpu.make_async_copy(vs[w], vb[w], in_sem.at[w + 6])

    def own(w, l, h, first=False):
        if w < DOWN:
            return pltpu.make_async_copy(cells[w][h].at[l], outs[w][h].at[l, x, y], own_sem.at[number(w, l, h)])
        src = new[h].at[l, pl.ds(0, 56) if first else pl.ds(8, 48)]
        return pltpu.make_async_copy(src, outs[DOWN][h].at[l, x, y, tiles(0, first)], own_sem.at[number(w, l, h)])

    def own_each(w, l, h, act):
        if w < DOWN:
            act(own(w, l, h))
        else:
            either(firsts[0], lambda: act(own(w, l, h, True)), lambda: act(own(w, l, h)))

    def optimizer(w, h):
        c = cols(w, h)

        grad, weight = (ref.at[:, :, pl.ds(0, COLS[w][h][1])] for ref in (total[w // 2], wide[w // 2]))
        for l in LAYERS:
            grad[l] = r3[w][h][l * 3 + 2].astype(F32)
            weight[l] = near[w][l, :, c].astype(F32)

        def one(r, _):
            row = pl.ds(r + 2 * z, 1)
            g = jnp.concatenate([grad[l, row, :] for l in LAYERS], 0)
            old = jnp.concatenate([weight[l, row, :] for l in LAYERS], 0)
            m = 0.9 * mb[w][r, :, c] + 0.1 * g
            v = 0.95 * vb[w][r, :, c] + 0.05 * g * g
            step = m * lax.rsqrt(v + 1e-8) + 0.1 * old
            out = old - 0.02 * step
            mo[w][r, :, c] = m
            vo[w][r, :, c] = v
            for l in LAYERS:
                weight[l, row, :] = out[l : l + 1]
            return 0

        lax.fori_loop(0, OWNED[w], one, 0)
        for l in LAYERS:
            to = ends[w][h].at[l, z] if w < DOWN else new[h].at[l]
            to[...] = weight[l].astype(BF16)

    def join(w, l, h):
        row = lax.broadcasted_iota(jnp.int32, (8, COLS[w][h][1]), 0)
        top = [ends[w][h][l, i, 0:8].astype(F32) for i in range(4)]
        low = [ends[w][h][l, i, 8:16].astype(F32) for i in range(4)]
        for i, tile in enumerate([top[0], *(jnp.where(row < DOWN * i, low[i - 1], top[i]) for i in (1, 2, 3)), low[3]]):
            cells[w][h][l, 8 * i : 8 * i + 8] = tile.astype(BF16)

    def mend(l, h):
        row = lax.broadcasted_iota(jnp.int32, (8, COLS[2][h][1]), 0)
        new[h][l, 48:56] = jnp.where(row < DOWN * z + 2, new[h][l, 48:56].astype(F32), edge[h][l].astype(F32)).astype(BF16)

    for copy in inputs():
        copy.start()
    for down in range(2):
        for n in range(LOADS[down]):
            load(down, n).start()
    barrier = pltpu.get_barrier_semaphore()
    for axis in AXES:
        for sign in SIGN:
            pl.semaphore_signal(barrier, inc=1, device_id=towards(axis, sign), device_id_type=LOGICAL)
    pl.semaphore_wait(barrier, 6)

    used, begun = [0, 0], False
    flying, staying = {}, {f for f in FLOWS if f[0] == 2}

    def key(m):
        return (*m[:4], m[5] if len(m) > 5 else 0)

    for kind, task in steps:
        if kind == "send":
            if key(task) in flying:
                gone(flying.pop(key(task)))
            if task[0] in "qr" and task[1] == DOWN and task[1:4] in staying:
                staying.remove(task[1:4])
                own_each(*task[1:4], lambda copy: copy.wait())
            start(task)
            flying[key(task)] = task
            continue
        if not begun:
            for copy in inputs():
                copy.wait()
            begun = True
        name, w, *rest = task
        if name == "step":
            optimizer(w, rest[0])
            continue
        came(task)
        l, h, t, *k = rest
        if name == "a":
            down = w // 2
            n = used[down]
            used[down] += 1
            load(down, n).wait()
            to = spot(r1, w, l, h, t, k[0])
            add_to(to, to, slot(w, h, n))
            if n + LOADS[down] < len(loads[down]):
                load(down, n + LOADS[down]).start()
        elif name == "b":
            to = spot(r2, w, l, h, t)
            add_to(to, to, spot(r1, w, l, h, 2, t + 1))
        elif name == "c":
            to = spot(r3, w, l, h, t)
            add_to(to, to, last(w, l, h, t))
        elif name == "e":
            gone(flying.pop(key(task)))
            mend(l, h)
            own_each(w, l, h, lambda copy: copy.start())
        elif name == "p" and t == 2 and w < DOWN:
            join(w, l, h)
            own_each(w, l, h, lambda copy: copy.start())
    for task in flying.values():
        gone(task)
    for w, l, h in FLOWS:
        if w < DOWN:
            own_each(w, l, h, lambda copy: copy.wait())


SHAPES = ((2, 4, 4, 40, 3200),) * 2 + ((2, 4, 4, 200, 640),)
MOMENTS = ((10, 2, 3200),) * 2 + ((50, 2, 640),)


def exchanged(*arrays):
    dma, vmem = pltpu.SemaphoreType.DMA, pltpu.VMEM
    flow = len(HALVES)
    ring_sems = [dma((6 * flow,)), dma((18 * flow,))]
    chunk_sems = [dma((24 * flow,)), dma((72 * flow,))]

    def halved(weights, shape, dtype=BF16):
        return [vmem((*shape(w), COLS[w][h][1]), dtype) for w in weights for h in HALVES]

    everything, wide, down = WEIGHTS, WEIGHTS[:DOWN], WEIGHTS[DOWN:]
    results = [vmem((*SHAPES[w][:4], COLS[w][h][1]), BF16) for w in everything for h in HALVES]
    return pl.pallas_call(
        kernel,
        out_shape=results + [vmem(s, F32) for s in MOMENTS * 2],
        in_specs=[IN_HBM] * 12,
        out_specs=[ANYWHERE] * (3 * flow) + [IN_VMEM] * 6,
        scratch_shapes=[
            *halved(everything, lambda w: (24, *((40,) if w < DOWN else (4, 56)))),
            *halved(everything, lambda w: (6, *((40,) if w < DOWN else (4, 56)))),
            *halved(everything, lambda w: (6, WINDOW[w])),
            vmem((LOADS[0], 40, COLS[0][0][1]), BF16),
            vmem((LOADS[1], 4, 56, COLS[2][0][1]), BF16),
            *(vmem((2, WINDOW[w], COLS[w][0][1]), F32) for w in (0, 2)),
            *(vmem((2, WINDOW[w], COLS[w][0][1]), F32) for w in (0, 2)),
            *(vmem((2, n, width), BF16) for n, width in zip(WINDOW, WIDTH, strict=True)),
            *(vmem(s, F32) for s in MOMENTS * 2),
            *halved(wide, lambda w: (2, 4, 16)),
            *halved(wide, lambda w: (2, 40)),
            *halved(down, lambda w: (2, 56)),
            *halved(down, lambda w: (2, 8)),
            *chunk_sems,
            *ring_sems,
            *ring_sems,
            dma((2 * flow,)),
            dma((2 * flow,)),
            *ring_sems,
            *ring_sems,
            *chunk_sems,
            dma((sum(LOADS),)),
            dma((9,)),
            dma((6 * flow,)),
        ],
        compiler_params=pltpu.CompilerParams(collective_id=0, has_side_effects=True, vmem_limit_bytes=33 * 2**20),
        name="sum_step_gather",
    )(*arrays)


def put_kernel(*refs):
    n = len(HALVES)
    ins, outs, sem = refs[: 3 * n + 6], refs[3 * n + 6 : -1], refs[-1]
    pairs = [(ins[w * n + h], outs[w].at[:, :, :, :, pl.ds(*COLS[w][h])]) for w in WEIGHTS for h in HALVES]
    pairs += zip(ins[3 * n :], outs[3:], strict=True)
    copies = [pltpu.make_async_copy(a, b, sem.at[i]) for i, (a, b) in enumerate(pairs)]
    for copy in copies:
        copy.start()
    for copy in copies:
        copy.wait()


def put(arrays):
    return pl.pallas_call(
        put_kernel,
        out_shape=[jax.ShapeDtypeStruct(s, BF16) for s in SHAPES] + [jax.ShapeDtypeStruct(s, F32) for s in MOMENTS * 2],
        in_specs=[ANYWHERE] * len(arrays),
        out_specs=[IN_HBM] * 9,
        scratch_shapes=[pltpu.SemaphoreType.DMA((len(arrays),))],
        compiler_params=pltpu.CompilerParams(vmem_limit_bytes=2**20),
        name="put",
    )(*arrays)


def solution(mesh):
    def step(*arrays):
        terms, weights, m, v = (arrays[i : i + 3] for i in (0, 3, 6, 9))
        cut = [a.reshape(s) for a, s in zip((*terms, *weights), SHAPES * 2, strict=True)]
        moments = [pltpu.with_memory_space_constraint(a.transpose(1, 0, 2), pltpu.HBM) for a in (*m, *v)]
        out = put(exchanged(*cut, *moments))
        return (*(o.reshape(w.shape) for o, w in zip(out, weights, strict=False)), *(o.transpose(1, 0, 2) for o in out[3:]))

    all_of, cut = P(None, None, None), P(None, "dp", None)
    return jax.shard_map(
        step,
        mesh=mesh,
        in_specs=(P(("rep", "dp"), None, None, None),) * 3 + (all_of,) * 3 + (cut,) * 6,
        out_specs=(P("rep", None, None),) * 3 + (P("rep", "dp", None),) * 6,
        check_vma=False,
    )
```

```python
import jax
import jax.numpy as jnp
from jax import lax
from jax.experimental import pallas as pl
from jax.experimental.pallas import tpu as pltpu
from jax.sharding import PartitionSpec as P

BF16, F32 = jnp.bfloat16, jnp.float32
LOGICAL = pl.DeviceIdType.LOGICAL
SIGN = (1, -1)
COLS = (((0, 1536), (1536, 1664)),) * 2 + (((0, 384), (384, 256)),)
HALVES = LAYERS = (0, 1)
WEIGHTS = AXES = HOPS = (0, 1, 2)
CHUNKS = (0, 1, 2, 3)
DOWN = 2
CELLS = (4,)
ALL = slice(None)
IN_HBM, IN_VMEM, ANYWHERE = (pl.BlockSpec(memory_space=space) for space in (pltpu.HBM, pltpu.VMEM, pl.ANY))
XYZ, YXZ, ZXY, ZYX = (0, 1, 2), (1, 0, 2), (2, 0, 1), (2, 1, 0)
ORDER = (((XYZ, XYZ),) * 2, ((YXZ, YXZ),) * 2, ((ZXY, ZYX),) * 2)
FLOWS = tuple((w, l, h) for h in HALVES for w in WEIGHTS for l in LAYERS)
CELL, OWNED, APART, WINDOW = (40, 40, 200), (10, 10, 50), (8, 8, 48), (16, 16, 56)
WIDTH = (3200, 3200, 640)
MOST = tuple(max(width for _, width in halves) for halves in COLS)


def cross(w, h):
    return w == 1 and h == 0


def back(w, l, h):
    one, two, three = ORDER[w][l][h]
    return (one, three, two) if cross(w, h) else (one, two, three)


def plan():
    ahead, rate, trip, little = 0.5, 44.0e3, 3.0, 0.05
    sizes, tasks = {}, {}
    for w, l, h in FLOWS:
        one, two, three = ((axis, l) for axis in ORDER[w][l][h])
        _, late, early = ((axis, l) for axis in back(w, l, h))
        width = COLS[w][h][1] * 2
        whole, part, last = width * (40 if w < DOWN else 224), width * (40 if w < DOWN else 192), width * WINDOW[w]
        add, four = 5 / 2 / 1024 / 1900, cross(w, h)
        for t in HOPS:
            on = t < 2
            for k in CHUNKS:
                a = ("a", w, l, h, t, k)
                sizes[a] = (one, whole, 1 + 0.5 * h - 0.1 * t)
                then = [("a", w, l, h, t + 1, k)] if on else [("b", w, l, h, 0)] if k == 0 else []
                then += [("a", w, l, h + 1, 0, k)] if t == 2 and h + 1 < len(HALVES) else []
                tasks[a] = (a, [], whole * add, then)
                r = ("r", w, l, h, t, k)
                sizes[r] = (one, part, 5 + -1 * h + 0 * t)
                tasks[r] = (r, [("q", w, l, h, 2)], little, [("r", w, l, h, t + 1, k)] if on else [])
            b, c, p, q = ((name, w, l, h, t) for name in "bcpq")
            sizes.update({b: (two, whole, 0), c: (three, last, 0), p: (early, last, -2), q: (late, width * 64 if four else part, 2 - 2 * h)})
            tasks[b] = (b, [("a", w, l, h, 2, t + 1)], whole * add, [("b", w, l, h, t + 1)] if on else [("c", w, l, h, 0)])
            tasks[c] = (c, [("b", w, l, h, 2)], last * add, [("c", w, l, h, t + 1)] if on else [])
            tasks[p] = (p, [("step", w, h)], little if on else 0.4, [("p", w, l, h, t + 1)] if on else [("q", w, l, h, 0)] + [("r", w, l, h, 0, 0)] * (not four))
            then = [("r", w, l, h, 0, k) for k in CHUNKS if t == 2] if four else [("r", w, l, h, 0, t + 1)]
            tasks[q] = (q, [("p", w, l, h, 2)], little, ([("q", w, l, h, t + 1)] if on else []) + then)
    for h in HALVES:
        for w in WEIGHTS:
            tasks["step", w, h] = (None, [("c", w, l, h, 2) for l in LAYERS], 1.5, [("p" if w < DOWN else "e", w, l, h, 0) for l in LAYERS])
        for l in LAYERS:
            e = ("e", 2, l, h, 0)
            sizes[e] = ((2, 1), 16 * COLS[2][h][1], 0)
            tasks[e] = (e, [("step", 2, h)], 0.1, [("p", 2, l, h, 0)])
    waiting, free, arrived, done, steps, count = {}, {}, {}, {}, [], 0

    def push(message):
        nonlocal count
        link, _, rank = sizes[message]
        waiting.setdefault(link, []).append((rank, count, message))
        waiting[link].sort()
        count += 1

    for k in CHUNKS:
        for w in WEIGHTS:
            for l in LAYERS:
                push(("a", w, l, 0, 0, k))
    now = 0.0
    while tasks:
        issued = True
        while issued:
            ready = []
            for place, (task, (message, before, _, _)) in enumerate(tasks.items()):
                if (message is None or message in arrived) and all(b in done for b in before):
                    ready.append((max([arrived.get(message, 0.0)] + [done[b] for b in before]), place, task))
            at, _, task = min(ready) if ready else (now + 9, 0, None)
            until, issued = max(now + ahead, at + 0.3), False
            for link in sorted(waiting):
                while waiting[link] and free.get(link, 0.0) < until:
                    message = waiting[link].pop(0)[2]
                    free[link] = max(free.get(link, 0.0), now) + sizes[message][1] / rate
                    arrived[message] = free[link] + trip
                    steps.append(("send", message))
                    issued = True
        _, _, time, then = tasks.pop(task)
        now = max(now, at) + time
        done[task] = now
        steps.append(("task", task))
        for message in then:
            push(message)
    return steps


def rows8(i, size):
    return pl.ds(pl.multiple_of(i, 8), size)


def over_rows(ref, body):
    if len(ref.shape) == 3:
        lax.fori_loop(0, ref.shape[0], lambda j, _: (body((j,)), 0)[1], 0)
    elif ref.shape[0] == 40:
        lax.fori_loop(0, 5, lambda j, _: (body((rows8(8 * j, 8),)), 0)[1], 0)
    else:
        body((ALL,))


def either(first, yes, no):
    def call(act):
        act()

    lax.cond(first, lambda: call(yes), lambda: call(no))


def add_to(out, a, b):
    def one(i):
        out[i] = (a[i].astype(F32) + b[i].astype(F32)).astype(BF16)

    over_rows(out, one)


LOADS = (8, 6)


def kernel(*refs):
    refs = list(refs)

    def take(n):
        taken = tuple(refs[:n])
        del refs[:n]
        return taken

    def halved(n):
        return [take(len(HALVES)) for _ in range(n)]

    terms, weights, ms, vs = (take(3) for _ in range(4))
    outs, mo, vo = halved(3), take(3), take(3)
    r1, r2, r3, held = halved(3), halved(3), halved(3), take(2)
    total, wide, near, mb, vb = take(2), take(2), take(3), take(3), take(3)
    ends, (new, edge) = halved(2), halved(2)
    a_send, a_recv, b_send, b_recv, c_send, c_recv, e_send, e_recv = take(8)
    p_send, p_recv, q_send, q_recv, r_send, r_recv = take(6)
    load_sem, in_sem, own_sem = take(3)

    me = lax.axis_index("dp")
    at = x, y, z = lax.div(me, 16), lax.rem(lax.div(me, 4), 4), lax.rem(me, 4)

    places = [[at[axis]] + [lax.rem(at[axis] + n, 4) for n in (1, 2, 3)] for axis in AXES]
    eights, windows, bands = ([[f(p) for p in places[axis]] for axis in AXES] for f in (lambda p: 8 * p, lambda p: 48 * p, lambda p: 48 * p + 8))
    firsts = [p == 0 for p in places[2]]
    next_to = {}
    for axis in AXES:
        for sign in SIGN:
            to = list(at)
            to[axis] = places[axis][sign % 4]
            next_to[axis, sign] = lax.axis_index("rep") * 64 + to[0] * 16 + to[1] * 4 + to[2]

    def towards(axis, sign):
        return next_to[axis, sign]

    def ring(axis, sign, steps, of=places):
        return of[axis][-sign * steps % 4]

    def number(w, l, h):
        return (w * 2 + l) * len(HALVES) + h

    def cols(w, h):
        return pl.ds(*COLS[w][h])

    def source(w, l, h, steps, k):
        a, b, _ = ORDER[w][l][h]
        chunk = ring(1 - a if w < DOWN else b, SIGN[l], 1 + k)
        if w < DOWN:
            block = ring(a, SIGN[l], steps)
            i, j = (block, chunk) if a == 0 else (chunk, block)
            return terms[w].at[l, i, j, :, cols(w, h)]
        window = rows8(ring(a, SIGN[l], steps, windows), 56)
        return terms[w].at[l, chunk, :, window, cols(w, h)] if b == 0 else terms[w].at[l, :, chunk, window, cols(w, h)]

    def slot(w, h, n):
        n = n % LOADS[w // 2]
        return held[0].at[n, :, pl.ds(0, COLS[w][h][1])] if w < DOWN else held[1].at[n, :, :, pl.ds(0, COLS[w][h][1])]

    steps = plan()
    loads = [[task for kind, task in steps if kind == "task" and task[0] == "a" and (task[1] == DOWN) == down] for down in (False, True)]

    def load(down, n):
        _, w, l, h, t, k = loads[down][n]
        return pltpu.make_async_copy(source(w, l, h, 2 + t, k), slot(w, h, n), load_sem.at[down * LOADS[0] + n % LOADS[down]])

    def spot(refs, w, l, h, t, k=None):
        return refs[w][h].at[l * 3 + t if k is None else l * 12 + t * 4 + k]

    def last(w, l, h, t):
        axis = ORDER[w][l][h][2]
        if w < DOWN:
            return r2[w][h].at[l * 3 + 2, rows8(ring(axis, SIGN[l], t + 2, eights), 16)]
        return r2[w][h].at[l * 3 + 2, ring(axis, SIGN[l], 2 + t)]

    def tiles(steps, first):
        return pl.ds(0, 56) if first else rows8(bands[2][-steps % 4], 48)

    def message(name, w, l, h, t, k=0, first=False):
        one, two, three = back(w, l, h) if name in "pqr" else ORDER[w][l][h]
        s, n = SIGN[l], number(w, l, h)
        if name == "a":
            axis, sems = one, (a_send.at[n * 4 + k], a_recv.at[n * 12 + t * 4 + k])
            dst = spot(r1, w, l, h, t, k)
            src = source(w, l, h, 1, k) if t == 0 else spot(r1, w, l, h, t - 1, k)
        elif name == "b":
            axis, sems = two, (b_send.at[n], b_recv.at[n * 3 + t])
            dst = spot(r2, w, l, h, t)
            src = spot(r1, w, l, h, 2, 0) if t == 0 else spot(r2, w, l, h, t - 1)
        elif name == "c":
            axis, sems = three, (c_send.at[n], c_recv.at[n * 3 + t])
            dst = spot(r3, w, l, h, t)
            src = last(w, l, h, -1) if t == 0 else spot(r3, w, l, h, t - 1)
        elif name == "e":
            axis, s, sems = 2, -1, (e_send.at[n], e_recv.at[n])
            src, dst = new[h].at[l, pl.ds(0, 8)], edge[h].at[l]
        elif name == "p":
            axis, sems = three, (p_send.at[n], p_recv.at[n * 3 + t])
            block = ring(three, s, t)
            if w < DOWN:
                src = dst = ends[w][h].at[l, block, z] if cross(w, h) else ends[w][h].at[l, block]
            else:
                i, j = (x, block) if three == 1 else (block, y)
                src = dst = outs[DOWN][h].at[l, i, j, tiles(0, first)]
                if t == 0:
                    src = new[h].at[l, pl.ds(0, 56) if first else pl.ds(8, 48)]
        elif name == "q":
            axis, sems = two, (q_send.at[n], q_recv.at[n * 3 + t])
            block = ring(two, s, t)
            if cross(w, h):
                src = dst = ends[w][h].at[l, :, block]
            elif w < DOWN:
                i, j = (x, block) if two == 1 else (block, y)
                src = dst = outs[w][h].at[l, i, j]
            else:
                i, j = (ALL, block) if two == 1 else (block, ALL)
                src = dst = outs[DOWN][h].at[l, i, j, tiles(0, first)]
        else:
            axis, sems = one, (r_send.at[n * 4 + k], r_recv.at[n * 12 + t * 4 + k])
            block, chunk = ring(one, s, t), ring(1 - one if w < DOWN else two, s, k)
            if w < DOWN:
                i, j = (block, chunk) if one == 0 else (chunk, block)
                src = dst = outs[w][h].at[l, i, j]
            else:
                i, j = (ALL, chunk) if two == 1 else (chunk, ALL)
                src = dst = outs[DOWN][h].at[l, i, j, tiles(s * t, first)]
        return pltpu.make_async_remote_copy(
            src_ref=src, dst_ref=dst, send_sem=sems[0], recv_sem=sems[1], device_id=towards(axis, s), device_id_type=LOGICAL
        )

    def each(m, act, coming=False):
        name, w, l, h, t = m[:5]
        if w < DOWN or name not in "pqr":
            act(message(*m))
            return
        first = firsts[0] if name != "r" else ring(0, SIGN[l], t + coming, [firsts])
        either(first, lambda: act(message(*m, first=True)), lambda: act(message(*m)))

    def start(m):
        each(m, lambda copy: copy.start())

    def came(m):
        name, w, l, h, t = m[:5]
        each(m, lambda copy: copy.wait_recv(), coming=True)

    def gone(m):
        each(m, lambda copy: copy.wait_send())

    def inputs():
        for w in WEIGHTS:
            yield pltpu.make_async_copy(weights[w].at[:, x, y, rows8(z * APART[w], WINDOW[w]), :], near[w], in_sem.at[w])
            yield pltpu.make_async_copy(ms[w], mb[w], in_sem.at[w + 3])
            yield pltpu.make_async_copy(vs[w], vb[w], in_sem.at[w + 6])

    def own(l, h, act):
        def copy(first):
            src = new[h].at[l, pl.ds(0, 56) if first else pl.ds(8, 48)]
            return pltpu.make_async_copy(src, outs[DOWN][h].at[l, x, y, tiles(0, first)], own_sem.at[l * len(HALVES) + h])

        either(firsts[0], lambda: act(copy(True)), lambda: act(copy(False)))

    def optimizer(w, h):
        c = cols(w, h)

        grad, weight = (ref.at[:, :, pl.ds(0, COLS[w][h][1])] for ref in (total[w // 2], wide[w // 2]))
        for l in LAYERS:
            grad[l] = r3[w][h][l * 3 + 2].astype(F32)
            weight[l] = near[w][l, :, c].astype(F32)

        def one(r, _):
            row = pl.ds(r + 2 * z, 1)
            g = jnp.concatenate([grad[l, row, :] for l in LAYERS], 0)
            old = jnp.concatenate([weight[l, row, :] for l in LAYERS], 0)
            m = 0.9 * mb[w][r, :, c] + 0.1 * g
            v = 0.95 * vb[w][r, :, c] + 0.05 * g * g
            step = m * lax.rsqrt(v + 1e-8) + 0.1 * old
            out = old - 0.02 * step
            mo[w][r, :, c] = m
            vo[w][r, :, c] = v
            for l in LAYERS:
                weight[l, row, :] = out[l : l + 1]
            return 0

        lax.fori_loop(0, OWNED[w], one, 0)
        for l in LAYERS:
            to = ends[w][h].at[(l, y if w == 0 else x, z) if cross(w, h) else (l, z)] if w < DOWN else new[h].at[l]
            to[...] = weight[l].astype(BF16)

    def join(w, l, h):
        row = lax.broadcasted_iota(jnp.int32, (8, COLS[w][h][1]), 0)

        def one(windows, *cell):
            top = [windows[i, 0:8].astype(F32) for i in CHUNKS]
            low = [windows[i, 8:16].astype(F32) for i in CHUNKS]
            for i, tile in enumerate([top[0], *(jnp.where(row < 2 * i, low[i - 1], top[i]) for i in CHUNKS[1:]), low[3]]):
                outs[w][h][l, *cell, 8 * i : 8 * i + 8] = tile.astype(BF16)

        def some(n, _):
            one(ends[w][h].at[l, n], *((x, n) if ORDER[w][l][h][0] == 0 else (n, y)))
            return 0

        if cross(w, h):
            lax.fori_loop(0, 4, some, 0)
        else:
            one(ends[w][h].at[l], x, y)

    def mend(l, h):
        row = lax.broadcasted_iota(jnp.int32, (8, COLS[2][h][1]), 0)
        new[h][l, 48:56] = jnp.where(row < DOWN * z + 2, new[h][l, 48:56].astype(F32), edge[h][l].astype(F32)).astype(BF16)

    for copy in inputs():
        copy.start()
    for down in range(2):
        for n in range(LOADS[down]):
            load(down, n).start()
    barrier = pltpu.get_barrier_semaphore()
    for axis in AXES:
        for sign in SIGN:
            pl.semaphore_signal(barrier, inc=1, device_id=towards(axis, sign), device_id_type=LOGICAL)
    pl.semaphore_wait(barrier, 6)

    used, begun = [0, 0], False
    flying, staying = {}, {f for f in FLOWS if f[0] == 2}

    def key(m):
        return (*m[:4], m[5] if len(m) > 5 else 0)

    for kind, task in steps:
        if kind == "send":
            if key(task) in flying:
                gone(flying.pop(key(task)))
            if task[0] in "qr" and task[1:4] in staying:
                staying.remove(task[1:4])
                own(*task[2:4], lambda copy: copy.wait())
            start(task)
            flying[key(task)] = task
            continue
        if not begun:
            for copy in inputs():
                copy.wait()
            begun = True
        name, w, *rest = task
        if name == "step":
            optimizer(w, rest[0])
            continue
        came(task)
        l, h, t, *k = rest
        if name == "a":
            down = w // 2
            n = used[down]
            used[down] += 1
            load(down, n).wait()
            to = spot(r1, w, l, h, t, k[0])
            add_to(to, to, slot(w, h, n))
            if n + LOADS[down] < len(loads[down]):
                load(down, n + LOADS[down]).start()
        elif name == "b":
            to = spot(r2, w, l, h, t)
            add_to(to, to, spot(r1, w, l, h, 2, t + 1))
        elif name == "c":
            to = spot(r3, w, l, h, t)
            add_to(to, to, last(w, l, h, t))
        elif name == "e":
            gone(flying.pop(key(task)))
            mend(l, h)
            own(l, h, lambda copy: copy.start())
        elif name == ("q" if cross(w, h) else "p") and t == 2 and w < DOWN:
            join(w, l, h)
    for task in flying.values():
        gone(task)


SHAPES = ((2, 4, 4, 40, 3200),) * 2 + ((2, 4, 4, 200, 640),)
MOMENTS = ((10, 2, 3200),) * 2 + ((50, 2, 640),)


def exchanged(*arrays):
    dma, vmem = pltpu.SemaphoreType.DMA, pltpu.VMEM
    flow = len(HALVES)
    ring_sems, chunk_sems = ([dma((n * len(FLOWS),)) for n in (each, 3 * each)] for each in (1, 4))

    def halved(weights, shape, dtype=BF16):
        return [vmem((*shape(w, cross(w, h)), COLS[w][h][1]), dtype) for w in weights for h in HALVES]

    everything, wide, down = WEIGHTS, WEIGHTS[:DOWN], WEIGHTS[DOWN:]
    results = [vmem((*SHAPES[w][:4], COLS[w][h][1]), BF16) for w in everything for h in HALVES]
    return pl.pallas_call(
        kernel,
        out_shape=results + [vmem(s, F32) for s in MOMENTS * 2],
        in_specs=[IN_HBM] * 12,
        out_specs=[IN_VMEM] * (3 * flow + 6),
        scratch_shapes=[
            *halved(everything, lambda w, four: (24, *((40,) if w < DOWN else (4, 56)))),
            *halved(everything, lambda w, four: (6, *((40,) if w < DOWN else (4, 56)))),
            *halved(everything, lambda w, four: (6, WINDOW[w])),
            vmem((LOADS[0], 40, MOST[0]), BF16),
            vmem((LOADS[1], 4, 56, MOST[DOWN]), BF16),
            *(vmem((2, WINDOW[w], MOST[w]), F32) for w in (0, 2)),
            *(vmem((2, WINDOW[w], MOST[w]), F32) for w in (0, 2)),
            *(vmem((2, n, width), BF16) for n, width in zip(WINDOW, WIDTH, strict=True)),
            *(vmem(s, F32) for s in MOMENTS * 2),
            *halved(wide, lambda w, four: (2, *CELLS[:four], 4, 16)),
            *halved(down, lambda w, four: (2, 56)),
            *halved(down, lambda w, four: (2, 8)),
            *chunk_sems,
            *ring_sems,
            *ring_sems,
            *ring_sems,
            *ring_sems,
            *ring_sems,
            *chunk_sems,
            dma((sum(LOADS),)),
            dma((9,)),
            dma((len(FLOWS),)),
        ],
        compiler_params=pltpu.CompilerParams(collective_id=0, has_side_effects=True, vmem_limit_bytes=35 * 2**20),
        name="sum_step_gather",
    )(*arrays)


def put_kernel(*refs):
    n = len(HALVES)
    ins, outs, sem = refs[: 3 * n + 6], refs[3 * n + 6 : -1], refs[-1]
    pairs = [(ins[w * n + h], outs[w].at[:, :, :, :, pl.ds(*COLS[w][h])]) for w in WEIGHTS for h in HALVES]
    pairs += zip(ins[3 * n :], outs[3:], strict=True)
    copies = [pltpu.make_async_copy(a, b, sem.at[i]) for i, (a, b) in enumerate(pairs)]
    for copy in copies:
        copy.start()
    for copy in copies:
        copy.wait()


def put(arrays):
    return pl.pallas_call(
        put_kernel,
        out_shape=[jax.ShapeDtypeStruct(s, BF16) for s in SHAPES] + [jax.ShapeDtypeStruct(s, F32) for s in MOMENTS * 2],
        in_specs=[ANYWHERE] * len(arrays),
        out_specs=[IN_HBM] * 9,
        scratch_shapes=[pltpu.SemaphoreType.DMA((len(arrays),))],
        compiler_params=pltpu.CompilerParams(vmem_limit_bytes=2**20),
        name="put",
    )(*arrays)


def solution(mesh):
    def step(*arrays):
        terms, weights, m, v = (arrays[i : i + 3] for i in (0, 3, 6, 9))
        cut = [a.reshape(s) for a, s in zip((*terms, *weights), SHAPES * 2, strict=True)]
        moments = [pltpu.with_memory_space_constraint(a.transpose(1, 0, 2), pltpu.HBM) for a in (*m, *v)]
        out = put(exchanged(*cut, *moments))
        return (*(o.reshape(w.shape) for o, w in zip(out, weights, strict=False)), *(o.transpose(1, 0, 2) for o in out[3:]))

    all_of, cut = P(None, None, None), P(None, "dp", None)
    return jax.shard_map(
        step,
        mesh=mesh,
        in_specs=(P(("rep", "dp"), None, None, None),) * 3 + (all_of,) * 3 + (cut,) * 6,
        out_specs=(P("rep", None, None),) * 3 + (P("rep", "dp", None),) * 6,
        check_vma=False,
    )
```

```python
import jax
import jax.numpy as jnp
from jax import lax
from jax.experimental import pallas as pl
from jax.experimental.pallas import tpu as pltpu
from jax.sharding import PartitionSpec as P

BF16, F32 = jnp.bfloat16, jnp.float32
LOGICAL = pl.DeviceIdType.LOGICAL
SIGN = (1, -1)
COLS = (((0, 1536), (1536, 1664)),) * 2 + (((0, 384), (384, 256)),)
HALVES = LAYERS = (0, 1)
WEIGHTS = AXES = HOPS = (0, 1, 2)
CHUNKS = (0, 1, 2, 3)
DOWN = 2
CELLS = (4,)
ALL = slice(None)
IN_HBM, IN_VMEM, ANYWHERE = (pl.BlockSpec(memory_space=space) for space in (pltpu.HBM, pltpu.VMEM, pl.ANY))
XYZ, YXZ, ZXY, ZYX = (0, 1, 2), (1, 0, 2), (2, 0, 1), (2, 1, 0)
ORDER = (((XYZ, XYZ),) * 2, ((YXZ, YXZ),) * 2, ((ZXY, ZYX),) * 2)
FLOWS = tuple((w, l, h) for h in HALVES for w in WEIGHTS for l in LAYERS)
CELL, OWNED, APART, WINDOW = (40, 40, 200), (10, 10, 50), (8, 8, 48), (16, 16, 56)
WIDTH = (3200, 3200, 640)
MOST = tuple(max(width for _, width in halves) for halves in COLS)


def cross(w, h):
    return w == 1 and h == 0


def back(w, l, h):
    one, two, three = ORDER[w][l][h]
    return (one, three, two) if cross(w, h) else (one, two, three)


def plan():
    ahead, rate, trip, little = 0.5, 44.0e3, 3.0, 0.05
    sizes, tasks = {}, {}
    for w, l, h in FLOWS:
        one, two, three = ((axis, l) for axis in ORDER[w][l][h])
        _, late, early = ((axis, l) for axis in back(w, l, h))
        width = COLS[w][h][1] * 2
        whole, part, last = width * (40 if w < DOWN else 224), width * (40 if w < DOWN else 192), width * WINDOW[w]
        add, four = 5 / 2 / 1024 / 1900, cross(w, h)
        for t in HOPS:
            on = t < 2
            for k in CHUNKS:
                a = ("a", w, l, h, t, k)
                sizes[a] = (one, whole, 1 + 0.5 * h - 0.1 * t)
                then = [("a", w, l, h, t + 1, k)] if on else [("b", w, l, h, 0)] if k == 0 else []
                then += [("a", w, l, h + 1, 0, k)] if t == 2 and h + 1 < len(HALVES) else []
                tasks[a] = (a, [], whole * add, then)
                r = ("r", w, l, h, t, k)
                sizes[r] = (one, part, 5 + -1 * h + 0 * t)
                tasks[r] = (r, [("q", w, l, h, 2)], little, [("r", w, l, h, t + 1, k)] if on else [])
            b, c, p, q = ((name, w, l, h, t) for name in "bcpq")
            sizes.update({b: (two, whole, 0), c: (three, last, 0), p: (early, last, -2), q: (late, width * 64 if four else part, 2 - 2 * h)})
            tasks[b] = (b, [("a", w, l, h, 2, t + 1)], whole * add, [("b", w, l, h, t + 1)] if on else [("c", w, l, h, 0)])
            tasks[c] = (c, [("b", w, l, h, 2)], last * add, [("c", w, l, h, t + 1)] if on else [])
            tasks[p] = (p, [("step", w, h)], little if on else 0.4, [("p", w, l, h, t + 1)] if on else [("q", w, l, h, 0)] + [("r", w, l, h, 0, 0)] * (not four))
            then = [("r", w, l, h, 0, k) for k in CHUNKS if t == 2] if four else [("r", w, l, h, 0, t + 1)]
            tasks[q] = (q, [("p", w, l, h, 2)], little, ([("q", w, l, h, t + 1)] if on else []) + then)
    for h in HALVES:
        for w in WEIGHTS:
            tasks["step", w, h] = (None, [("c", w, l, h, 2) for l in LAYERS], 1.5, [("p" if w < DOWN else "e", w, l, h, 0) for l in LAYERS])
        for l in LAYERS:
            e = ("e", 2, l, h, 0)
            sizes[e] = ((2, 1), 16 * COLS[2][h][1], 0)
            tasks[e] = (e, [("step", 2, h)], 0.1, [("p", 2, l, h, 0)])
    waiting, free, arrived, done, steps, count = {}, {}, {}, {}, [], 0

    def push(message):
        nonlocal count
        link, _, rank = sizes[message]
        waiting.setdefault(link, []).append((rank, count, message))
        waiting[link].sort()
        count += 1

    for k in CHUNKS:
        for w in WEIGHTS:
            for l in LAYERS:
                push(("a", w, l, 0, 0, k))
    now = 0.0
    while tasks:
        issued = True
        while issued:
            ready = []
            for place, (task, (message, before, _, _)) in enumerate(tasks.items()):
                if (message is None or message in arrived) and all(b in done for b in before):
                    ready.append((max([arrived.get(message, 0.0)] + [done[b] for b in before]), place, task))
            at, _, task = min(ready) if ready else (now + 9, 0, None)
            until, issued = max(now + ahead, at + 0.3), False
            for link in sorted(waiting):
                while waiting[link] and free.get(link, 0.0) < until:
                    message = waiting[link].pop(0)[2]
                    free[link] = max(free.get(link, 0.0), now) + sizes[message][1] / rate
                    arrived[message] = free[link] + trip
                    steps.append(("send", message))
                    issued = True
        _, _, time, then = tasks.pop(task)
        now = max(now, at) + time
        done[task] = now
        steps.append(("task", task))
        for message in then:
            push(message)
    return steps


def rows8(i, size):
    return pl.ds(pl.multiple_of(i, 8), size)


def over_rows(ref, body):
    if len(ref.shape) == 3:
        lax.fori_loop(0, ref.shape[0], lambda j, _: (body((j,)), 0)[1], 0)
    elif ref.shape[0] == 40:
        lax.fori_loop(0, 5, lambda j, _: (body((rows8(8 * j, 8),)), 0)[1], 0)
    else:
        body((ALL,))


def either(first, yes, no):
    def call(act):
        act()

    lax.cond(first, lambda: call(yes), lambda: call(no))


def add_to(out, a, b):
    def one(i):
        out[i] = (a[i].astype(F32) + b[i].astype(F32)).astype(BF16)

    over_rows(out, one)


LOADS = (8, 6)


def kernel(*refs):
    refs = list(refs)

    def take(n):
        taken = tuple(refs[:n])
        del refs[:n]
        return taken

    def halved(n):
        return [take(len(HALVES)) for _ in range(n)]

    terms, weights, ms, vs = (take(3) for _ in range(4))
    outs, mo, vo = halved(3), take(3), take(3)
    r1, r2, r3, held = halved(3), halved(3), halved(3), take(2)
    total, wide, near, mb, vb = take(2), take(2), take(3), take(3), take(3)
    ends, (new, edge) = halved(2), halved(2)
    a_send, a_recv, b_send, b_recv, c_send, c_recv, e_send, e_recv = take(8)
    p_send, p_recv, q_send, q_recv, r_send, r_recv = take(6)
    load_sem, in_sem, own_sem = take(3)

    me = lax.axis_index("dp")
    at = x, y, z = lax.div(me, 16), lax.rem(lax.div(me, 4), 4), lax.rem(me, 4)

    places = [[at[axis]] + [lax.rem(at[axis] + n, 4) for n in (1, 2, 3)] for axis in AXES]
    eights, windows, bands = ([[f(p) for p in places[axis]] for axis in AXES] for f in (lambda p: 8 * p, lambda p: 48 * p, lambda p: 48 * p + 8))
    firsts = [p == 0 for p in places[2]]
    next_to = {}
    for axis in AXES:
        for sign in SIGN:
            to = list(at)
            to[axis] = places[axis][sign % 4]
            next_to[axis, sign] = lax.axis_index("rep") * 64 + to[0] * 16 + to[1] * 4 + to[2]

    def towards(axis, sign):
        return next_to[axis, sign]

    def ring(axis, sign, steps, of=places):
        return of[axis][-sign * steps % 4]

    def number(w, l, h):
        return (w * 2 + l) * len(HALVES) + h

    def cols(w, h):
        return pl.ds(*COLS[w][h])

    def source(w, l, h, steps, k):
        a, b, _ = ORDER[w][l][h]
        chunk = ring(1 - a if w < DOWN else b, SIGN[l], 1 + k)
        if w < DOWN:
            block = ring(a, SIGN[l], steps)
            i, j = (block, chunk) if a == 0 else (chunk, block)
            return terms[w].at[l, i, j, :, cols(w, h)]
        window = rows8(ring(a, SIGN[l], steps, windows), 56)
        return terms[w].at[l, chunk, :, window, cols(w, h)] if b == 0 else terms[w].at[l, :, chunk, window, cols(w, h)]

    def slot(w, h, n):
        n = n % LOADS[w // 2]
        return held[0].at[n, :, pl.ds(0, COLS[w][h][1])] if w < DOWN else held[1].at[n, :, :, pl.ds(0, COLS[w][h][1])]

    steps = plan()
    loads = [[task for kind, task in steps if kind == "task" and task[0] == "a" and (task[1] == DOWN) == down] for down in (False, True)]

    def load(down, n):
        _, w, l, h, t, k = loads[down][n]
        return pltpu.make_async_copy(source(w, l, h, 2 + t, k), slot(w, h, n), load_sem.at[down * LOADS[0] + n % LOADS[down]])

    def spot(refs, w, l, h, t, k=None):
        return refs[w][h].at[l * 3 + t if k is None else l * 12 + t * 4 + k]

    def last(w, l, h, t):
        axis = ORDER[w][l][h][2]
        if w < DOWN:
            return r2[w][h].at[l * 3 + 2, rows8(ring(axis, SIGN[l], t + 2, eights), 16)]
        return r2[w][h].at[l * 3 + 2, ring(axis, SIGN[l], 2 + t)]

    def tiles(steps, first):
        return pl.ds(0, 56) if first else rows8(bands[2][-steps % 4], 48)

    def message(name, w, l, h, t, k=0, first=False):
        one, two, three = back(w, l, h) if name in "pqr" else ORDER[w][l][h]
        s, n = SIGN[l], number(w, l, h)
        if name == "a":
            axis, sems = one, (a_send.at[n * 4 + k], a_recv.at[n * 12 + t * 4 + k])
            dst = spot(r1, w, l, h, t, k)
            src = source(w, l, h, 1, k) if t == 0 else spot(r1, w, l, h, t - 1, k)
        elif name == "b":
            axis, sems = two, (b_send.at[n], b_recv.at[n * 3 + t])
            dst = spot(r2, w, l, h, t)
            src = spot(r1, w, l, h, 2, 0) if t == 0 else spot(r2, w, l, h, t - 1)
        elif name == "c":
            axis, sems = three, (c_send.at[n], c_recv.at[n * 3 + t])
            dst = spot(r3, w, l, h, t)
            src = last(w, l, h, -1) if t == 0 else spot(r3, w, l, h, t - 1)
        elif name == "e":
            axis, s, sems = 2, -1, (e_send.at[n], e_recv.at[n])
            src, dst = new[h].at[l, pl.ds(0, 8)], edge[h].at[l]
        elif name == "p":
            axis, sems = three, (p_send.at[n], p_recv.at[n * 3 + t])
            block = ring(three, s, t)
            if w < DOWN:
                src = dst = ends[w][h].at[l, block, z] if cross(w, h) else ends[w][h].at[l, block]
            else:
                i, j = (x, block) if three == 1 else (block, y)
                src = dst = outs[DOWN][h].at[l, i, j, tiles(0, first)]
                if t == 0:
                    src = new[h].at[l, pl.ds(0, 56) if first else pl.ds(8, 48)]
        elif name == "q":
            axis, sems = two, (q_send.at[n], q_recv.at[n * 3 + t])
            block = ring(two, s, t)
            if cross(w, h):
                src = dst = ends[w][h].at[l, :, block]
            elif w < DOWN:
                i, j = (x, block) if two == 1 else (block, y)
                src = dst = outs[w][h].at[l, i, j]
            else:
                i, j = (ALL, block) if two == 1 else (block, ALL)
                src = dst = outs[DOWN][h].at[l, i, j, tiles(0, first)]
        else:
            axis, sems = one, (r_send.at[n * 4 + k], r_recv.at[n * 12 + t * 4 + k])
            block, chunk = ring(one, s, t), ring(1 - one if w < DOWN else two, s, k)
            if w < DOWN:
                i, j = (block, chunk) if one == 0 else (chunk, block)
                src = dst = outs[w][h].at[l, i, j]
            else:
                i, j = (ALL, chunk) if two == 1 else (chunk, ALL)
                src = dst = outs[DOWN][h].at[l, i, j, tiles(s * t, first)]
        return pltpu.make_async_remote_copy(
            src_ref=src, dst_ref=dst, send_sem=sems[0], recv_sem=sems[1], device_id=towards(axis, s), device_id_type=LOGICAL
        )

    def each(m, act, coming=False):
        name, w, l, h, t = m[:5]
        if w < DOWN or name not in "pqr":
            act(message(*m))
            return
        first = firsts[0] if name != "r" else ring(0, SIGN[l], t + coming, [firsts])
        either(first, lambda: act(message(*m, first=True)), lambda: act(message(*m)))

    def start(m):
        each(m, lambda copy: copy.start())

    def came(m):
        name, w, l, h, t = m[:5]
        each(m, lambda copy: copy.wait_recv(), coming=True)

    def gone(m):
        each(m, lambda copy: copy.wait_send())

    def inputs():
        for w in WEIGHTS:
            yield pltpu.make_async_copy(weights[w].at[:, x, y, rows8(z * APART[w], WINDOW[w]), :], near[w], in_sem.at[w])
            yield pltpu.make_async_copy(ms[w], mb[w], in_sem.at[w + 3])
            yield pltpu.make_async_copy(vs[w], vb[w], in_sem.at[w + 6])

    def own(l, h, act):
        def copy(first):
            src = new[h].at[l, pl.ds(0, 56) if first else pl.ds(8, 48)]
            return pltpu.make_async_copy(src, outs[DOWN][h].at[l, x, y, tiles(0, first)], own_sem.at[l * len(HALVES) + h])

        either(firsts[0], lambda: act(copy(True)), lambda: act(copy(False)))

    def optimizer(w, h):
        c = cols(w, h)

        grad, weight = (ref.at[:, :, pl.ds(0, COLS[w][h][1])] for ref in (total[w // 2], wide[w // 2]))
        for l in LAYERS:
            grad[l] = r3[w][h][l * 3 + 2].astype(F32)
            weight[l] = near[w][l, :, c].astype(F32)

        def one(r, _):
            row = pl.ds(r + 2 * z, 1)
            g = jnp.concatenate([grad[l, row, :] for l in LAYERS], 0)
            old = jnp.concatenate([weight[l, row, :] for l in LAYERS], 0)
            m = 0.9 * mb[w][r, :, c] + 0.1 * g
            v = 0.95 * vb[w][r, :, c] + 0.05 * g * g
            step = m * lax.rsqrt(v + 1e-8) + 0.1 * old
            out = old - 0.02 * step
            mo[w][r, :, c] = m
            vo[w][r, :, c] = v
            for l in LAYERS:
                weight[l, row, :] = out[l : l + 1]
            return 0

        lax.fori_loop(0, OWNED[w], one, 0)
        for l in LAYERS:
            to = ends[w][h].at[(l, y if w == 0 else x, z) if cross(w, h) else (l, z)] if w < DOWN else new[h].at[l]
            to[...] = weight[l].astype(BF16)

    def join(w, l, h):
        row = lax.broadcasted_iota(jnp.int32, (8, COLS[w][h][1]), 0)

        def one(windows, *cell):
            top = [windows[i, 0:8].astype(F32) for i in CHUNKS]
            low = [windows[i, 8:16].astype(F32) for i in CHUNKS]
            for i, tile in enumerate([top[0], *(jnp.where(row < 2 * i, low[i - 1], top[i]) for i in CHUNKS[1:]), low[3]]):
                outs[w][h][l, *cell, 8 * i : 8 * i + 8] = tile.astype(BF16)

        def some(n, _):
            one(ends[w][h].at[l, n], *((x, n) if ORDER[w][l][h][0] == 0 else (n, y)))
            return 0

        if cross(w, h):
            lax.fori_loop(0, 4, some, 0)
        else:
            one(ends[w][h].at[l], x, y)

    def mend(l, h):
        row = lax.broadcasted_iota(jnp.int32, (8, COLS[2][h][1]), 0)
        new[h][l, 48:56] = jnp.where(row < DOWN * z + 2, new[h][l, 48:56].astype(F32), edge[h][l].astype(F32)).astype(BF16)

    for copy in inputs():
        copy.start()
    for down in range(2):
        for n in range(LOADS[down]):
            load(down, n).start()
    barrier = pltpu.get_barrier_semaphore()
    for axis in AXES:
        for sign in SIGN:
            pl.semaphore_signal(barrier, inc=1, device_id=towards(axis, sign), device_id_type=LOGICAL)
    pl.semaphore_wait(barrier, 6)

    used, begun = [0, 0], False
    flying, staying = {}, {f for f in FLOWS if f[0] == 2}

    def key(m):
        return (*m[:4], m[5] if len(m) > 5 else 0)

    for kind, task in steps:
        if kind == "send":
            if key(task) in flying:
                gone(flying.pop(key(task)))
            if task[0] in "qr" and task[1:4] in staying:
                staying.remove(task[1:4])
                own(*task[2:4], lambda copy: copy.wait())
            start(task)
            flying[key(task)] = task
            continue
        if not begun:
            for copy in inputs():
                copy.wait()
            begun = True
        name, w, *rest = task
        if name == "step":
            optimizer(w, rest[0])
            continue
        came(task)
        l, h, t, *k = rest
        if name == "a":
            down = w // 2
            n = used[down]
            used[down] += 1
            load(down, n).wait()
            to = spot(r1, w, l, h, t, k[0])
            add_to(to, to, slot(w, h, n))
            if n + LOADS[down] < len(loads[down]):
                load(down, n + LOADS[down]).start()
        elif name == "b":
            to = spot(r2, w, l, h, t)
            add_to(to, to, spot(r1, w, l, h, 2, t + 1))
        elif name == "c":
            to = spot(r3, w, l, h, t)
            add_to(to, to, last(w, l, h, t))
        elif name == "e":
            gone(flying.pop(key(task)))
            mend(l, h)
            own(l, h, lambda copy: copy.start())
        elif name == ("q" if cross(w, h) else "p") and t == 2 and w < DOWN:
            join(w, l, h)
    for task in flying.values():
        gone(task)


SHAPES = ((2, 4, 4, 40, 3200),) * 2 + ((2, 4, 4, 200, 640),)
MOMENTS = ((10, 2, 3200),) * 2 + ((50, 2, 640),)


def exchanged(*arrays):
    dma, vmem = pltpu.SemaphoreType.DMA, pltpu.VMEM
    flow = len(HALVES)
    ring_sems, chunk_sems = ([dma((n * len(FLOWS),)) for n in (each, 3 * each)] for each in (1, 4))

    def halved(weights, shape, dtype=BF16):
        return [vmem((*shape(w, cross(w, h)), COLS[w][h][1]), dtype) for w in weights for h in HALVES]

    everything, wide, down = WEIGHTS, WEIGHTS[:DOWN], WEIGHTS[DOWN:]
    results = [vmem((*SHAPES[w][:4], COLS[w][h][1]), BF16) for w in everything for h in HALVES]
    return pl.pallas_call(
        kernel,
        out_shape=results + [vmem(s, F32) for s in MOMENTS * 2],
        in_specs=[IN_HBM] * 12,
        out_specs=[IN_VMEM] * (3 * flow + 6),
        scratch_shapes=[
            *halved(everything, lambda w, four: (24, *((40,) if w < DOWN else (4, 56)))),
            *halved(everything, lambda w, four: (6, *((40,) if w < DOWN else (4, 56)))),
            *halved(everything, lambda w, four: (6, WINDOW[w])),
            vmem((LOADS[0], 40, MOST[0]), BF16),
            vmem((LOADS[1], 4, 56, MOST[DOWN]), BF16),
            *(vmem((2, WINDOW[w], MOST[w]), F32) for w in (0, 2)),
            *(vmem((2, WINDOW[w], MOST[w]), F32) for w in (0, 2)),
            *(vmem((2, n, width), BF16) for n, width in zip(WINDOW, WIDTH, strict=True)),
            *(vmem(s, F32) for s in MOMENTS * 2),
            *halved(wide, lambda w, four: (2, *CELLS[:four], 4, 16)),
            *halved(down, lambda w, four: (2, 56)),
            *halved(down, lambda w, four: (2, 8)),
            *chunk_sems,
            *ring_sems,
            *ring_sems,
            *ring_sems,
            *ring_sems,
            *ring_sems,
            *chunk_sems,
            dma((sum(LOADS),)),
            dma((9,)),
            dma((len(FLOWS),)),
        ],
        compiler_params=pltpu.CompilerParams(collective_id=0, has_side_effects=True, vmem_limit_bytes=35 * 2**20),
        name="sum_step_gather",
    )(*arrays)


def put_kernel(*refs):
    n = len(HALVES)
    ins, outs, sem = refs[: 3 * n + 6], refs[3 * n + 6 : -1], refs[-1]
    pairs = [(ins[w * n + h].at[l], outs[w].at[l, :, :, :, pl.ds(*COLS[w][h])]) for w in WEIGHTS for h in HALVES for l in LAYERS]
    pairs += zip(ins[3 * n :], outs[3:], strict=True)
    copies = [pltpu.make_async_copy(a, b, sem.at[i]) for i, (a, b) in enumerate(pairs)]
    for copy in copies:
        copy.start()
    for copy in copies:
        copy.wait()


def put(arrays):
    return pl.pallas_call(
        put_kernel,
        out_shape=[jax.ShapeDtypeStruct(s, BF16) for s in SHAPES] + [jax.ShapeDtypeStruct(s, F32) for s in MOMENTS * 2],
        in_specs=[ANYWHERE] * len(arrays),
        out_specs=[IN_HBM] * 9,
        scratch_shapes=[pltpu.SemaphoreType.DMA((2 * len(arrays),))],
        compiler_params=pltpu.CompilerParams(vmem_limit_bytes=2**20),
        name="put",
    )(*arrays)


def solution(mesh):
    def step(*arrays):
        terms, weights, m, v = (arrays[i : i + 3] for i in (0, 3, 6, 9))
        cut = [a.reshape(s) for a, s in zip((*terms, *weights), SHAPES * 2, strict=True)]
        moments = [pltpu.with_memory_space_constraint(a.transpose(1, 0, 2), pltpu.HBM) for a in (*m, *v)]
        out = put(exchanged(*cut, *moments))
        return (*(o.reshape(w.shape) for o, w in zip(out, weights, strict=False)), *(o.transpose(1, 0, 2) for o in out[3:]))

    all_of, cut = P(None, None, None), P(None, "dp", None)
    return jax.shard_map(
        step,
        mesh=mesh,
        in_specs=(P(("rep", "dp"), None, None, None),) * 3 + (all_of,) * 3 + (cut,) * 6,
        out_specs=(P("rep", None, None),) * 3 + (P("rep", "dp", None),) * 6,
        check_vma=False,
    )
```
